32 devices in a mesh: slab: 4 (over x, core), rep: 8 (over z, y).
Axes of the slice: x: 2, y: 2, z: 4, core: 2. Of those that a mesh axis runs over, the one named last changes fastest.
Arguments:
- image: float32 [144, 256, 256], P('slab', 'rep'), may hold values from 0.5 to 2
- sensitivity: float32 [144, 256, 256], P('slab', 'rep'), may hold values from 0.5 to 2
- system_blocks: bfloat16 [512, 128, 1024], P(('slab', 'rep')), may hold values from 0 to 0.00390625
- tile_slab: int32 [512, 1], P(('slab', 'rep')), may hold values from 0 to 3; in each aligned block of 16 rows (0 to 15, 16 to 31, ...) at most 6 rows name the same one
- tile_block: int32 [512], P(('slab', 'rep')), may hold values from 0 to 2303
- background: bfloat16 [512, 128], P(('slab', 'rep')), may hold values from 0.19921875 to 1
Outputs:
- updated: float32 [144, 256, 256], P('slab', 'rep')
The draws below stay inside these ranges and needn't reach their ends.
Inputs may be any that keep to these rules, and one draw needn't show every extreme that they name: `tile_slab`: among the 16 tiles of one device at most 6 view the same slab, and in some devices some slab is viewed by exactly 6.
All inputs are finite; a program needn't handle non-finite values.
Results may differ from the reference program's by a relative error of at most 0.0003.
Values may be sent and summed in bfloat16 or wider, within the bound.
A program may use at most 64 MiB of HBM per device.

```python
import math
import jax
import jax.numpy as jnp
import numpy as np
from jax import lax

NX = 256
NY = 256
TILE = 128
VB = 1024
PIECES_PER_CARD = 16
CAP = 6
NZ = 144
NBLK = 2304
TILES = 512
N_SLAB = 4


def place_ends(entries, own_key, smallest, largest):
    dims = entries.shape
    place = [jax.random.randint(jax.random.fold_in(own_key, axis), (), 0, dims[axis]) for axis in range(len(dims))]
    entries = entries.at[tuple(place)].set(smallest)
    longest = dims.index(max(dims))
    place[longest] = (place[longest] + 1) % dims[longest]
    return entries.at[tuple(place)].set(largest)


def level_of(rng, dims, pieces, low, top_value):
    def one(axis_at, blocks):
        draws = jax.random.uniform(jax.random.fold_in(jax.random.fold_in(rng, 6), axis_at), (blocks,), jnp.float32, low / len(pieces), top_value / len(pieces))
        return jnp.repeat(jnp.exp(draws), dims[axis_at] // blocks).reshape((-1,) + (1,) * (len(dims) - axis_at - 1))

    level = one(*pieces[0])
    for cut in pieces[1:]:
        level = level * one(*cut)
    return level


def assign_block(key, own, number, rows, amount, top, limit, skew):
    ranking = jax.random.permutation(key, amount)
    heavy_load, ordinary = portions_of(amount, rows * top, limit, skew, True), portions_of(amount, rows * top, limit, skew, False)
    places = jnp.arange(amount)

    def named(sizes, turn):
        used = int((sizes > 0).sum())
        fixed = max(1, used // 4)
        shifted = fixed + (places - fixed + turn * (used - fixed)) % max(1, amount - fixed)
        return jnp.zeros((amount,), jnp.int32).at[ranking[jnp.where(places < fixed, places, shifted)]].set(jnp.asarray(sizes, jnp.int32))

    sizes = jnp.where(number % 4 == 0, named(heavy_load, number // 4), named(ordinary, number - number // 4 - 1))
    mixed = jax.random.permutation(jax.random.fold_in(own, 3), amount)
    giver, sink = mixed[0:amount // 2 * 2:2], mixed[1:amount // 2 * 2:2]
    margin = jnp.minimum(sizes[giver] - 1, limit - sizes[sink]) // 2
    margin = jnp.where((giver == ranking[0]) | (sink == ranking[0]) | (sizes[sink] == 0), 0, jnp.maximum(margin, 0))
    shifted = jax.random.randint(jax.random.fold_in(own, 4), (amount // 2,), 0, 1 << 20) % (margin + 1)
    sizes = sizes.at[giver].add(-shifted).at[sink].add(shifted)
    labels = jnp.searchsorted(jnp.cumsum(sizes), jnp.arange(rows * top), side="right").astype(jnp.int32)
    listing = labels.reshape(top, rows).T
    listing = listing[jax.random.permutation(jax.random.fold_in(own, 1), rows)]
    turn = jax.random.randint(jax.random.fold_in(own, 2), (rows, 1), 0, top)
    return jnp.take_along_axis(listing, (jnp.arange(top)[None, :] + turn) % top, axis=1)


def portions_of(count, total, reach, skew, full):
    portions = [(1 << 20) // math.isqrt(standing ** skew) + 1 for standing in range(1, count + 1)]
    largest = reach if full else min(reach, max(-(-total // count), total * portions[0] // sum(portions)))
    least = 1 if total - largest >= count - 1 else 0
    given, surplus = [largest] + [least] * (count - 1), total - largest - least * (count - 1)
    while surplus > 0:
        free = [i for i in range(1, count) if given[i] < largest] or [i for i in range(1, count) if given[i] < reach]
        whole, remaining = sum([portions[i] for i in free]), surplus
        for i in free:
            more = min(reach - given[i], max(1, remaining * portions[i] // whole), surplus)
            given[i] = given[i] + more
            surplus = surplus - more
    return np.array(given)


def setup_inputs(seed: int = 0) -> dict:
    splits = jax.random.split(jax.random.key(seed), 7)
    image = jnp.clip(jnp.exp(math.log(2.0) - 1.3862944 * jax.random.uniform(splits[0], (NZ, NY, NX), jnp.float32) ** level_of(splits[0], (NZ, NY, NX), ((0, 4), (1, 8)), -0.2, 0.2)), 0.5, 2.0)
    sensitivity = jnp.clip(jnp.exp(math.log(2.0) - 1.3862944 * jax.random.uniform(splits[1], (NZ, NY, NX), jnp.float32) ** level_of(splits[1], (NZ, NY, NX), ((0, 4), (1, 8)), -0.2, 0.2)), 0.5, 2.0)
    system_blocks = jnp.clip(0.00390625 * jax.random.uniform(splits[2], (TILES, TILE, VB), jnp.float32) ** level_of(splits[2], (TILES, TILE, VB), ((0, 32),), -0.2, 0.2), 0.0, 0.00390625).astype(jnp.bfloat16)
    tile_slab_keys = jax.random.split(jax.random.fold_in(splits[3], 1), TILES // PIECES_PER_CARD)
    tile_slab_turns = jax.random.permutation(jax.random.fold_in(splits[3], 3), TILES // PIECES_PER_CARD)
    tile_slab = jax.vmap(lambda own, number: assign_block(jax.random.fold_in(splits[3], 2), own, number, PIECES_PER_CARD, N_SLAB, 1, CAP, 2))(tile_slab_keys, tile_slab_turns).reshape((TILES, 1))
    tile_block = place_ends(jax.random.randint(splits[4], (TILES,), 0, NBLK), jax.random.fold_in(splits[4], 1), 0, NBLK - 1).astype(jnp.int32)
    background = jnp.clip(jnp.exp(math.log(1.0) - 1.6133518 * jax.random.uniform(splits[5], (TILES, TILE), jnp.float32) ** level_of(splits[5], (TILES, TILE), ((0, 32),), -0.2, 0.2)), 0.19921875, 1.0).astype(jnp.bfloat16)
    return dict(image=image, sensitivity=sensitivity, system_blocks=system_blocks, tile_slab=tile_slab, tile_block=tile_block, background=background)


def reference(image, sensitivity, system_blocks, tile_slab, tile_block, background):
    tile_rows = system_blocks.shape[1]
    width = system_blocks.shape[2]
    unrolled_emission_map = image.astype(jnp.bfloat16).reshape(-1, width)
    index = (tile_slab[:, 0].astype(jnp.int32) * NBLK + tile_block.astype(jnp.int32)).astype(jnp.int32)

    def one_group(group):
        response_operator_lines, rows_index, back_ground = group
        emission_cell_entries = unrolled_emission_map[rows_index].astype(jnp.float32)
        sys_wide = response_operator_lines.astype(jnp.float32)
        forward_projection = jnp.einsum('tev,tv->te', sys_wide, emission_cell_entries, precision=lax.Precision.HIGHEST)
        inverse_permutation = (1.0 / (forward_projection + back_ground.astype(jnp.float32))).astype(jnp.bfloat16)
        inverse_permutation = lax.optimization_barrier(inverse_permutation)
        return jnp.einsum('tev,te->tv', sys_wide, inverse_permutation.astype(jnp.float32), precision=lax.Precision.HIGHEST)

    groups = (system_blocks.reshape(-1, 16, tile_rows, width), index.reshape(-1, 16), background.reshape(-1, 16, tile_rows))
    backproj = lax.map(one_group, groups).reshape(-1, width)
    partial_value = jnp.zeros(unrolled_emission_map.shape, jnp.float32).at[index].add(backproj)
    return image * partial_value.reshape(image.shape) / sensitivity
```

```python
import functools

import jax
import jax.numpy as jnp
from jax import lax
from jax.experimental import pallas as pl
from jax.experimental.pallas import tpu as pltpu
from jax.sharding import PartitionSpec as P

CAP = 6
MAIN = 4
LEVELS = 65535.0
HALF = 32768
LANES = 128
MESH = pl.DeviceIdType.MESH


def split(x, size):
    if size & (size - 1):
        return x // size, x % size
    return x >> (size.bit_length() - 1), x & (size - 1)


def exchange_kernel(
    sizes, slab_hbm, block_hbm, image_hbm, sys_hbm, bg_hbm, asked_hbm, scale_ref, back_ref, more_ref,
    asked_ref, slab_v, block_v, bg_v, scale_v, image_v, blocks_v, sys_v, mine_v, slot_v, mine_s, slot_s, asked_s, send_f, recv_f, sums_v, bp_v, send_b,
    local_sem, id_sem, fetch_sem, back_sem, scale_sem,
):
    n, reps, tiles, block_rows, per_owner, low, high = sizes
    wide = high - low
    me = lax.axis_index("slab") * reps + lax.axis_index("rep")
    lane_tiles = image_v.shape[1] // LANES

    def device(d):
        return (lax.div(d, reps), lax.rem(d, reps))

    load_sys = pltpu.make_async_copy(sys_hbm, sys_v, local_sem.at[0])
    load_image = pltpu.make_async_copy(image_hbm, image_v, local_sem.at[1])
    load_slab = pltpu.make_async_copy(slab_hbm, slab_v, local_sem.at[4])
    load_block = pltpu.make_async_copy(block_hbm, block_v, local_sem.at[5])
    load_bg = pltpu.make_async_copy(bg_hbm, bg_v, local_sem.at[6])
    for load in (load_slab, load_block, load_image, load_bg, load_sys):
        load.start()

    barrier = pltpu.get_barrier_semaphore()

    def greet(i, c):
        pl.semaphore_signal(barrier, inc=1, device_id=device(lax.rem(me + i, n)), device_id_type=MESH)
        return c

    lax.fori_loop(1, n, greet, 0)

    load_slab.wait()
    load_block.wait()
    block = block_v[...]
    plane, within = split(block, per_owner * reps)
    owner, offset = split(within, per_owner)
    key = slab_v[...] * reps + owner
    value = (plane * per_owner + offset) * tiles + lax.broadcasted_iota(jnp.int32, (1, tiles), 1) + 1
    hot = key == lax.broadcasted_iota(jnp.int32, (n, tiles), 0)
    square = (tiles, tiles)
    earlier = lax.broadcasted_iota(jnp.int32, square, 0) < lax.broadcasted_iota(jnp.int32, square, 1)
    rank = jnp.dot(
        jnp.where(hot, 1.0, 0.0).astype(jnp.bfloat16),
        jnp.where(earlier, 1.0, 0.0).astype(jnp.bfloat16),
        preferred_element_type=jnp.float32,
    ).astype(jnp.int32)
    lane = lax.broadcasted_iota(jnp.int32, (n, LANES), 1)

    def tabled(row, zero):
        table = jnp.full((n, LANES), zero)
        for k in range(wide):
            picked = jnp.sum(jnp.where(hot & (rank == low + k), row, zero), axis=1, keepdims=True)
            table = jnp.where(lane == k, picked, table)
        return table

    own_rank = jnp.sum(jnp.where(hot, rank, 0), axis=0, keepdims=True)
    over = jnp.max(own_rank, axis=1, keepdims=True) // high
    mine_v[...] = jnp.where(lane == wide, jnp.minimum(over, 1), tabled(value, jnp.int32(0)))
    away = key - me
    slot = jnp.where(away < 0, away + n, away) * wide + own_rank - low
    slot_v[0:1, 0:tiles] = jnp.clip(slot, 0, n * wide - 1)
    to_slot = pltpu.make_async_copy(slot_v, slot_s, local_sem.at[2])
    to_slot.start()
    to_mine = pltpu.make_async_copy(mine_v, mine_s, local_sem.at[3])
    to_mine.start()
    asked_ref[pl.ds(0, 1), :] = mine_v[pl.ds(me, 1), :]

    pl.semaphore_wait(barrier, n - 1)

    def id_copy(i):
        d = lax.rem(me + i, n)
        return pltpu.make_async_remote_copy(
            src_ref=mine_v.at[pl.ds(d, 1)], dst_ref=asked_ref.at[pl.ds(i, 1)],
            send_sem=id_sem.at[0], recv_sem=id_sem.at[1],
            device_id=device(d), device_id_type=MESH,
        )

    def send_ids(i, c):
        id_copy(i).start()
        return c

    lax.fori_loop(1, n, send_ids, 0)
    to_slot.wait()
    to_mine.wait()
    load_image.wait()
    per_group = 8 // block_rows

    def cut(g, c):
        rows = image_v[pl.ds(pl.multiple_of(g * 8, 8), 8), :].astype(jnp.bfloat16).astype(jnp.float32)
        for u in range(per_group):
            blocks_v[g * per_group + u] = jnp.concatenate(
                [
                    rows[u * block_rows:(u + 1) * block_rows, h * LANES:(h + 1) * LANES]
                    for h in range(lane_tiles)
                ],
                axis=0,
            ).astype(jnp.bfloat16)
        return c

    lax.fori_loop(0, image_v.shape[0] // 8, cut, 0, unroll=4)
    rest = asked_ref.at[pl.ds(1, n - 1)]
    pltpu.make_async_copy(rest, rest, id_sem.at[1]).wait()
    to_asked = pltpu.make_async_copy(asked_ref, asked_s, local_sem.at[2])
    to_asked.start()
    keep_asked = pltpu.make_async_copy(asked_ref, asked_hbm, local_sem.at[3])
    keep_asked.start()
    to_asked.wait()

    more_ref[0] = lax.fori_loop(0, n, lambda i, c: jnp.maximum(c, asked_s[i, wide]), jnp.int32(0), unroll=4)

    def served(i, k):
        return blocks_v[split(jnp.maximum(asked_s[i, k] - 1, 0), tiles)[0]]

    for k in range(wide):
        recv_f[k] = served(0, k)

    def far_first(j):
        return lax.rem(j, slabs) * reps + lax.rem(reps // 2 + lax.div(j, slabs), reps)

    slabs = n // reps
    own_turn = (reps - reps // 2) * slabs

    def serve(j, c):
        i = far_first(j)
        for k in range(wide):
            send_f[i * wide + k] = served(i, k)
        span = pl.ds(i * wide, wide)
        pltpu.make_async_remote_copy(
            src_ref=send_f.at[span], dst_ref=recv_f.at[span],
            send_sem=fetch_sem.at[0], recv_sem=fetch_sem.at[1],
            device_id=device(lax.rem(me + n - i, n)), device_id_type=MESH,
        ).start()
        return c

    lax.fori_loop(0, own_turn, serve, 0)
    lax.fori_loop(own_turn + 1, n, serve, 0)
    load_bg.wait()
    background = jnp.transpose(bg_v[...].astype(jnp.float32))
    load_sys.wait()
    others = recv_f.at[pl.ds(wide, (n - 1) * wide)]
    pltpu.make_async_copy(others, others, fetch_sem.at[1]).wait()

    forward = jnp.zeros(background.shape, jnp.float32)
    tile_lane = lax.broadcasted_iota(jnp.int32, (1, tiles), 1)
    pieces = block_rows * lane_tiles
    places = [(p % block_rows) * lane_tiles + p // block_rows for p in range(pieces)]
    for t in range(tiles):
        cells = recv_f[slot_s[0, t]].astype(jnp.float32)
        total = None
        for p, q in enumerate(places):
            term = sys_v[t, :, q * LANES:(q + 1) * LANES].astype(jnp.float32) * cells[p:p + 1, :]
            total = term if total is None else total + term
        forward = jnp.where(tile_lane == t, jnp.sum(total, axis=1, keepdims=True), forward)
    inverse = jnp.transpose(1.0 / (forward + background)).astype(jnp.bfloat16)
    tops = []
    for t in range(tiles):
        back = jnp.dot(inverse, sys_v[t], preferred_element_type=jnp.float32)
        tile = jnp.concatenate([back[t:t + 1, q * LANES:(q + 1) * LANES] for q in places], axis=0)
        sums_v[t] = tile
        tops.append(jnp.max(tile, axis=0, keepdims=True))
    peak = jnp.maximum(jnp.max(jnp.concatenate(tops, axis=0), axis=1, keepdims=True), 1e-33)
    gain = LEVELS / peak
    peaks = jnp.transpose(peak)
    for t in range(tiles):
        level = jnp.round(sums_v[t] * gain[t:t + 1, :]).astype(jnp.int32) - HALF
        bp_v[t] = jnp.clip(level, -HALF, HALF - 1).astype(jnp.int16)
    scale_v[...] = tabled(peaks * (1.0 / LEVELS), jnp.float32(0))

    def routed(d, k):
        return bp_v[split(jnp.maximum(mine_s[d, k] - 1, 0), tiles)[1]]

    for k in range(wide):
        send_b[k] = routed(me, k)
    own_back = pltpu.make_async_copy(send_b.at[pl.ds(0, wide)], back_ref.at[pl.ds(0, wide)], local_sem.at[4])
    own_back.start()
    own_scale = pltpu.make_async_copy(scale_v.at[pl.ds(me, 1)], scale_ref.at[pl.ds(0, 1)], local_sem.at[5])
    own_scale.start()

    def give(j, c):
        i = far_first(j)
        d = lax.rem(me + i, n)
        for k in range(wide):
            send_b[i * wide + k] = routed(d, k)
        span = pl.ds(i * wide, wide)
        pltpu.make_async_remote_copy(
            src_ref=send_b.at[span], dst_ref=back_ref.at[span],
            send_sem=back_sem.at[0], recv_sem=back_sem.at[1],
            device_id=device(d), device_id_type=MESH,
        ).start()
        pltpu.make_async_remote_copy(
            src_ref=scale_v.at[pl.ds(d, 1)], dst_ref=scale_ref.at[pl.ds(i, 1)],
            send_sem=scale_sem.at[0], recv_sem=scale_sem.at[1],
            device_id=device(d), device_id_type=MESH,
        ).start()
        return c

    lax.fori_loop(0, own_turn, give, 0)
    lax.fori_loop(own_turn + 1, n, give, 0)
    for copy in (keep_asked, own_back, own_scale):
        copy.wait()
    scaled = scale_ref.at[pl.ds(1, n - 1)]
    pltpu.make_async_copy(scaled, scaled, scale_sem.at[0]).wait()
    pltpu.make_async_copy(scaled, scaled, scale_sem.at[1]).wait()
    pltpu.make_async_copy(mine_v.at[pl.ds(1, n - 1)], mine_v.at[pl.ds(1, n - 1)], id_sem.at[0]).wait()
    sent = send_f.at[pl.ds(wide, (n - 1) * wide)]
    pltpu.make_async_copy(sent, sent, fetch_sem.at[0]).wait()
    given = send_b.at[pl.ds(wide, (n - 1) * wide)]
    pltpu.make_async_copy(given, given, back_sem.at[0]).wait()
    landed = back_ref.at[pl.ds(wide, (n - 1) * wide)]
    pltpu.make_async_copy(landed, landed, back_sem.at[1]).wait()


def update_kernel(
    sizes, *refs,
):
    n, tiles, block_rows, widths = sizes
    parts = 3 * len(widths)
    out_hbm = refs[parts + 2]
    staged = refs[parts + 3:2 * parts + 5]
    image_ref, sens_ref = staged[parts:]
    out_ref, sums_v, in_sem, out_sem = refs[2 * parts + 5:]
    moves = tuple(zip(refs[:parts + 2], staged))
    loads = [pltpu.make_async_copy(src, dst, in_sem.at[j]) for j, (src, dst) in enumerate(moves)]
    for load in loads:
        load.start()
    lane_tiles = out_ref.shape[1] // LANES
    per_group = 8 // block_rows
    sums_v[...] = jnp.zeros_like(sums_v)

    for load in loads[:parts]:
        load.wait()
    for j, wide in enumerate(widths):
        asked_s, scale_s, back_ref = staged[3 * j:3 * j + 3]

        def add(i, k):
            if k == wide:
                return
            value = asked_s[i, k]

            @pl.when(value > 0)
            def _():
                level = back_ref[i * wide + k].astype(jnp.int32) + HALF
                sums_v[split(value - 1, tiles)[0]] += level.astype(jnp.float32) * scale_s[i, k]
                add(i, k + 1)

        def one(i, c):
            add(i, 0)
            return c

        lax.fori_loop(0, n, one, 0)
    for load in loads[parts:]:
        load.wait()

    def finish(g, c):
        rows = pl.ds(pl.multiple_of(g * 8, 8), 8)
        sums = [sums_v[g * per_group + u] for u in range(per_group)]
        for h in range(lane_tiles):
            cols = slice(h * LANES, (h + 1) * LANES)
            total = jnp.concatenate([s[h * block_rows:(h + 1) * block_rows] for s in sums], axis=0)
            out_ref[rows, cols] = image_ref[rows, cols] * total / sens_ref[rows, cols]
        return c

    groups = out_ref.shape[0] // 8
    chunks = out_sem.shape[0]
    stores = []
    for c in range(chunks):
        first, last = groups * c // chunks, groups * (c + 1) // chunks
        lax.fori_loop(first, last, finish, 0, unroll=4)
        span = pl.ds(first * 8, (last - first) * 8)
        stores.append(pltpu.make_async_copy(out_ref.at[span], out_hbm.at[span], out_sem.at[c]))
        stores[-1].start()
    for store in stores:
        store.wait()


def local(image, sensitivity, system_blocks, tile_slab, tile_block, background):
    slabs, reps = lax.axis_size("slab"), lax.axis_size("rep")
    n = slabs * reps
    tiles, events, width = system_blocks.shape
    planes, rows, cols = image.shape
    block_rows = width // cols
    per_owner = rows // block_rows
    image2 = image.reshape(planes * rows, cols)
    sens2 = sensitivity.reshape(planes * rows, cols)
    sub = width // LANES

    hbm = pl.BlockSpec(memory_space=pltpu.HBM)
    scalar = pl.BlockSpec(memory_space=pltpu.SMEM)

    def exchange(low, high):
        wide = high - low
        return pl.pallas_call(
            functools.partial(exchange_kernel, (n, reps, tiles, block_rows, per_owner, low, high)),
            out_shape=(
                jax.ShapeDtypeStruct((n, LANES), jnp.int32),
                jax.ShapeDtypeStruct((n, LANES), jnp.float32),
                jax.ShapeDtypeStruct((n * wide, sub, LANES), jnp.int16),
                jax.ShapeDtypeStruct((1,), jnp.int32),
            ),
            in_specs=[hbm] * 5,
            out_specs=(hbm, hbm, hbm, scalar),
            scratch_shapes=[
                pltpu.VMEM((n, LANES), jnp.int32),
                pltpu.VMEM((1, tiles), jnp.int32),
                pltpu.VMEM((1, tiles), jnp.int32),
                pltpu.VMEM(background.shape, jnp.bfloat16),
                pltpu.VMEM((n, LANES), jnp.float32),
                pltpu.VMEM(image2.shape, jnp.float32),
                pltpu.VMEM((planes * per_owner, sub, LANES), jnp.bfloat16),
                pltpu.VMEM(system_blocks.shape, jnp.bfloat16),
                pltpu.VMEM((n, LANES), jnp.int32),
                pltpu.VMEM((8, LANES), jnp.int32),
                pltpu.SMEM((n, LANES), jnp.int32),
                pltpu.SMEM((8, LANES), jnp.int32),
                pltpu.SMEM((n, LANES), jnp.int32),
                pltpu.VMEM((n * wide, sub, LANES), jnp.bfloat16),
                pltpu.VMEM((n * wide, sub, LANES), jnp.bfloat16),
                pltpu.VMEM((tiles, sub, LANES), jnp.float32),
                pltpu.VMEM((tiles, sub, LANES), jnp.int16),
                pltpu.VMEM((n * wide, sub, LANES), jnp.int16),
                pltpu.SemaphoreType.DMA((7,)),
                pltpu.SemaphoreType.DMA((2,)),
                pltpu.SemaphoreType.DMA((2,)),
                pltpu.SemaphoreType.DMA((2,)),
                pltpu.SemaphoreType.DMA((2,)),
            ],
            compiler_params=pltpu.CompilerParams(
                collective_id=min(low, 1), has_side_effects=True, vmem_limit_bytes=67043328
            ),
        )(tile_slab.reshape(1, tiles), tile_block.reshape(1, tiles), image2, system_blocks, background)

    def update(*parts):
        tables = [table for part in parts for table in part]
        widths = tuple(part[2].shape[0] // n for part in parts)
        staged = []
        for asked, scale, back in parts:
            staged += [
                pltpu.SMEM(asked.shape, jnp.int32),
                pltpu.SMEM(scale.shape, jnp.float32),
                pltpu.VMEM(back.shape, back.dtype),
            ]
        return pl.pallas_call(
            functools.partial(update_kernel, (n, tiles, block_rows, widths)),
            out_shape=jax.ShapeDtypeStruct(image2.shape, jnp.float32),
            in_specs=[hbm] * (len(tables) + 2),
            out_specs=hbm,
            scratch_shapes=[
                *staged,
                pltpu.VMEM(image2.shape, jnp.float32),
                pltpu.VMEM(image2.shape, jnp.float32),
                pltpu.VMEM(image2.shape, jnp.float32),
                pltpu.VMEM((planes * per_owner, sub, LANES), jnp.float32),
                pltpu.SemaphoreType.DMA((len(tables) + 2,)),
                pltpu.SemaphoreType.DMA((4,)),
            ],
            compiler_params=pltpu.CompilerParams(vmem_limit_bytes=67043328),
        )(*tables, image2, sens2)

    *main, more = exchange(0, MAIN)
    if MAIN == CAP:
        return update(main).reshape(image.shape)
    updated = lax.cond(
        more[0] > 0,
        lambda: update(main, exchange(MAIN, CAP)[:3]),
        lambda: update(main),
    )
    return updated.reshape(image.shape)


def solution(mesh):
    return jax.shard_map(
        local,
        mesh=mesh,
        in_specs=(
            P("slab", "rep", None),
            P("slab", "rep", None),
            P(("slab", "rep"), None, None),
            P(("slab", "rep"), None),
            P(("slab", "rep")),
            P(("slab", "rep"), None),
        ),
        out_specs=P("slab", "rep", None),
        check_vma=False,
    )
```

```python
import functools

import jax
import jax.numpy as jnp
from jax import lax
from jax.experimental import pallas as pl
from jax.experimental.pallas import tpu as pltpu
from jax.sharding import PartitionSpec as P

CAP = 6
MAIN = ((0, 1), (1, 4))
REST = ((4, CAP),)
LEVELS = 65535.0
HALF = 32768
LANES = 128
SUBLANES = 8
MESH = pl.DeviceIdType.MESH
VMEM_LIMIT = 32 * 1024 * 1024


def split(x, size):
    if size & (size - 1):
        return x // size, x % size
    return x >> (size.bit_length() - 1), x & (size - 1)


def listed(tiles, part):
    lo, hi = part
    return tiles if lo == 0 else tiles * (hi - lo) // hi


def padded(count):
    return -(-count // SUBLANES) * SUBLANES


def exchange_kernel(sizes, parts, *refs):
    n, reps, tiles, block_rows, per_owner = sizes
    low, high = parts[0][0], parts[-1][1]
    wide = high - low
    slab_hbm, block_hbm, image_hbm, sens_hbm, sys_hbm, bg_hbm, entry_ref, scale_ref, back_ref, ratio_ref, more_hbm = refs[:11]
    (
        more_s, asked_ref, slab_v, block_v, bg_v, scale_v, image_v, sens_v, blocks_v, sys_v, mine_v, list_v, mine_s, list_s, asked_s, sums_v,
        local_sem, id_sem, scale_sem, fetch_sem, back_sem,
    ) = refs[11:32]
    per_part = [refs[32 + 4 * c:36 + 4 * c] for c in range(len(parts))]
    me = lax.axis_index("slab") * reps + lax.axis_index("rep")
    lane_tiles = image_v.shape[1] // LANES

    def device(d):
        return (lax.div(d, reps), lax.rem(d, reps))

    def ahead_by(i):
        return lax.rem(me + i, n)

    load_sys = pltpu.make_async_copy(sys_hbm, sys_v, local_sem.at[0])
    load_image = pltpu.make_async_copy(image_hbm, image_v, local_sem.at[1])
    load_slab = pltpu.make_async_copy(slab_hbm, slab_v, local_sem.at[4])
    load_block = pltpu.make_async_copy(block_hbm, block_v, local_sem.at[5])
    load_bg = pltpu.make_async_copy(bg_hbm, bg_v, local_sem.at[6])
    load_sens = pltpu.make_async_copy(sens_hbm, sens_v, local_sem.at[4])
    for load in (load_slab, load_block, load_image, load_bg, load_sys):
        load.start()

    slabs = n // reps

    def each_partner(body):
        def line(j, carry):
            for s in range(slabs):
                body(s * reps + lax.rem(reps // 2 + j, reps))
            return carry

        far = reps - reps // 2
        lax.fori_loop(0, far, line, 0)
        for s in range(1, slabs):
            body(s * reps)
        lax.fori_loop(far + 1, reps, line, 0)

    barrier = pltpu.get_barrier_semaphore()

    def greet(i):
        pl.semaphore_signal(barrier, inc=1, device_id=device(ahead_by(i)), device_id_type=MESH)

    each_partner(greet)
    load_slab.wait()
    load_block.wait()
    load_sens.start()
    block = block_v[...]
    plane, within = split(block, per_owner * reps)
    owner, offset = split(within, per_owner)
    key = slab_v[...] * reps + owner
    tile_lane = lax.broadcasted_iota(jnp.int32, (1, tiles), 1)
    value = (plane * per_owner + offset) * tiles + 1
    hot = key == lax.broadcasted_iota(jnp.int32, (n, tiles), 0)
    square = (tiles, tiles)
    earlier = lax.broadcasted_iota(jnp.int32, square, 0) < lax.broadcasted_iota(jnp.int32, square, 1)
    earlier = jnp.where(earlier, 1.0, 0.0).astype(jnp.bfloat16)

    def before(mask):
        ones = jnp.where(mask, 1.0, 0.0).astype(jnp.bfloat16)
        return jnp.dot(ones, earlier, preferred_element_type=jnp.float32).astype(jnp.int32)

    rank = before(hot)
    lane = lax.broadcasted_iota(jnp.int32, (n, LANES), 1)

    def tabled(row, part, table):
        for k in range(*part):
            picked = jnp.sum(jnp.where(hot & (rank == k), row, jnp.zeros_like(row)), axis=1, keepdims=True)
            table = jnp.where(lane == k - low, picked, table)
        return table

    own_rank = jnp.sum(jnp.where(hot, rank, 0), axis=0, keepdims=True)
    over = jnp.max(jnp.where(own_rank >= high, 1, 0), axis=1, keepdims=True)
    table = jnp.where(lane == wide, over, 0)
    hots = []
    for c, (lo, hi) in enumerate(parts):
        slot = jnp.where(key < me, key - me + n, key - me) * (hi - lo) + own_rank - lo
        slot = jnp.clip(slot, 0, n * (hi - lo) - 1)
        row = 3 * SUBLANES * c
        if lo == 0:
            list_v[row:row + 1, 0:tiles] = slot
            hots.append(None)
            table = tabled(value + tile_lane, (lo, hi), table)
            continue
        room = padded(listed(tiles, (lo, hi)))
        mask = (own_rank >= lo) & (own_rank < hi)
        place = before(jnp.broadcast_to(mask, (room, tiles)))
        pick = (place == lax.broadcasted_iota(jnp.int32, (room, tiles), 0)) & mask
        hots.append(pick)
        tile_of = jnp.sum(jnp.where(pick, tile_lane, 0), axis=1, keepdims=True)
        slot_of = jnp.sum(jnp.where(pick, slot, 0), axis=1, keepdims=True)
        spread = lax.broadcasted_iota(jnp.int32, (room, LANES), 1)
        table = tabled(value + jnp.clip(place[0:1], 0, room - 1), (lo, hi), table)
        list_v[row + SUBLANES:row + SUBLANES + room, :] = jnp.where(spread == 0, jnp.minimum(tile_of, tiles - 1), jnp.minimum(slot_of, n * (hi - lo) - 1))
    mine_v[...] = table
    to_list = pltpu.make_async_copy(list_v, list_s, local_sem.at[2])
    to_list.start()
    to_mine = pltpu.make_async_copy(mine_v, mine_s, local_sem.at[3])
    to_mine.start()
    asked_ref[pl.ds(0, 1), :] = mine_v[pl.ds(me, 1), :]

    pl.semaphore_wait(barrier, n - 1)

    def send_ids(i):
        d = ahead_by(i)
        pltpu.make_async_remote_copy(
            src_ref=mine_v.at[pl.ds(d, 1)], dst_ref=asked_ref.at[pl.ds(i, 1)],
            send_sem=id_sem.at[0], recv_sem=id_sem.at[1],
            device_id=device(d), device_id_type=MESH,
        ).start()

    each_partner(send_ids)
    to_list.wait()
    to_mine.wait()
    load_image.wait()
    per_group = SUBLANES // block_rows

    def cut(g, c):
        rows = image_v[pl.ds(pl.multiple_of(g * SUBLANES, SUBLANES), SUBLANES), :].astype(jnp.bfloat16).astype(jnp.float32)
        for u in range(per_group):
            blocks_v[g * per_group + u] = jnp.concatenate(
                [
                    rows[u * block_rows:(u + 1) * block_rows, h * LANES:(h + 1) * LANES]
                    for h in range(lane_tiles)
                ],
                axis=0,
            ).astype(jnp.bfloat16)
        return c

    groups = image_v.shape[0] // SUBLANES
    lax.fori_loop(0, groups, cut, 0, unroll=4)
    load_sens.wait()

    def divide(g, c):
        rows = pl.ds(pl.multiple_of(g * SUBLANES, SUBLANES), SUBLANES)
        ratio_ref[rows, :] = image_v[rows, :] / sens_v[rows, :]
        return c

    lax.fori_loop(0, groups, divide, 0, unroll=4)
    load_bg.wait()
    background = bg_v[...]
    columns = []
    for pick in hots:
        if pick is None:
            columns.append(jnp.transpose(background.astype(jnp.float32)))
        else:
            ones = jnp.where(pick, 1.0, 0.0)
            chosen = jnp.dot(ones.astype(jnp.bfloat16), background, preferred_element_type=jnp.float32)
            columns.append(jnp.transpose(chosen + (1.0 - jnp.sum(ones, axis=1, keepdims=True))))
    load_sys.wait()
    rest = asked_ref.at[pl.ds(1, n - 1)]
    pltpu.make_async_copy(rest, rest, id_sem.at[1]).wait()
    to_asked = pltpu.make_async_copy(asked_ref, asked_s, local_sem.at[2])
    to_asked.start()
    to_asked.wait()

    def served(i, k):
        return blocks_v[split(jnp.maximum(asked_s[i, k] - 1, 0), tiles)[0]]

    def fetch(c):
        lo, hi = parts[c]
        span, (send_f, recv_f, _, _) = hi - lo, per_part[c]
        for k in range(span):
            recv_f[k] = served(0, lo - low + k)

        def serve(i):
            for k in range(span):
                send_f[i * span + k] = served(i, lo - low + k)
            at = pl.ds(i * span, span)
            pltpu.make_async_remote_copy(
                src_ref=send_f.at[at], dst_ref=recv_f.at[at],
                send_sem=fetch_sem.at[2 * c], recv_sem=fetch_sem.at[2 * c + 1],
                device_id=device(ahead_by(n - i)), device_id_type=MESH,
            ).start()

        each_partner(serve)

    for c in range(len(parts)):
        fetch(c)
    more_s[0] = lax.fori_loop(0, n, lambda i, m: jnp.maximum(m, asked_s[i, wide]), jnp.int32(0), unroll=4)
    keep_more = pltpu.make_async_copy(more_s, more_hbm, local_sem.at[3])
    keep_more.start()
    asked = asked_ref[...]
    below = lax.broadcasted_iota(jnp.int32, (n, n), 0) > lax.broadcasted_iota(jnp.int32, (n, n), 1)
    used = jnp.where((asked > 0) & (lane < wide), 1.0, 0.0).astype(jnp.bfloat16)
    ahead = jnp.dot(jnp.where(below, 1.0, 0.0).astype(jnp.bfloat16), used, preferred_element_type=jnp.float32).astype(jnp.int32)
    source = lax.broadcasted_iota(jnp.int32, (n, 1), 0)
    room = entry_ref.shape[1]
    position = lax.broadcasted_iota(jnp.int32, (n, room), 1)
    filled = jnp.zeros((1, 1), jnp.int32)
    entries = [jnp.zeros((1, room), jnp.int32) for _ in range(3)]
    for lo, hi in parts:
        for k in range(lo - low, hi - low):
            value_k = asked[:, k:k + 1]
            mine_k = (position == ahead[:, k:k + 1] + filled) & (value_k > 0)
            row_k = (lo - low) * n + source * (hi - lo) + k - (lo - low)
            facts = (row_k, split(value_k - 1, tiles)[0], source * wide + k)
            for f, fact in enumerate(facts):
                entries[f] += jnp.sum(jnp.where(mine_k, fact, 0), axis=0, keepdims=True)
            filled += jnp.sum(jnp.where(value_k > 0, 1, 0), axis=0, keepdims=True)
    for f, fact in enumerate(entries + [jnp.broadcast_to(filled, (1, room))]):
        entry_ref[f:f + 1, :] = fact

    pieces = block_rows * lane_tiles
    places = [(p % block_rows) * lane_tiles + p // block_rows for p in range(pieces)]
    scales = jnp.zeros((n, LANES), jnp.float32)
    for c, (lo, hi) in enumerate(parts):
        span, (send_f, recv_f, bp_v, send_b) = hi - lo, per_part[c]
        others = recv_f.at[pl.ds(span, (n - 1) * span)]
        pltpu.make_async_copy(others, others, fetch_sem.at[2 * c + 1]).wait()
        row, pick, count = 3 * SUBLANES * c, hots[c], listed(tiles, (lo, hi))
        if pick is None:
            chosen, cells_of = list(range(tiles)), [list_s[row, t] for t in range(tiles)]
        else:
            chosen = [jnp.clip(list_s[row + SUBLANES + j, 0], 0, tiles - 1) for j in range(count)]
            cells_of = [jnp.clip(list_s[row + SUBLANES + j, 1], 0, n * span - 1) for j in range(count)]
        forward = jnp.zeros(columns[c].shape, jnp.float32)
        column = lax.broadcasted_iota(jnp.int32, (1, forward.shape[1]), 1)
        for j in range(count):
            t = chosen[j]
            cells = recv_f[cells_of[j]].astype(jnp.float32)
            total = None
            for p, q in enumerate(places):
                term = sys_v[t, :, q * LANES:(q + 1) * LANES].astype(jnp.float32) * cells[p:p + 1, :]
                total = term if total is None else total + term
            forward = jnp.where(column == j, jnp.sum(total, axis=1, keepdims=True), forward)
        inverse = jnp.transpose(1.0 / (forward + columns[c])).astype(jnp.bfloat16)
        tops = []
        for j in range(count):
            back = jnp.dot(inverse, sys_v[chosen[j]], preferred_element_type=jnp.float32)
            tile = jnp.concatenate([back[j:j + 1, q * LANES:(q + 1) * LANES] for q in places], axis=0)
            sums_v[j] = tile
            tops.append(jnp.max(tile, axis=0, keepdims=True))
        peak = jnp.maximum(jnp.max(jnp.concatenate(tops, axis=0), axis=1, keepdims=True), 1e-33)
        gain = LEVELS / peak
        for j in range(count):
            level = jnp.round(sums_v[j] * gain[j:j + 1, :]).astype(jnp.int32) - HALF
            bp_v[j] = jnp.clip(level, -HALF, HALF - 1).astype(jnp.int16)

        def routed(d, k):
            return bp_v[split(jnp.maximum(mine_s[d, lo - low + k] - 1, 0), tiles)[1]]

        def give(i):
            d = ahead_by(i)
            for k in range(span):
                send_b[i * span + k] = routed(d, k)
            pltpu.make_async_remote_copy(
                src_ref=send_b.at[pl.ds(i * span, span)], dst_ref=back_ref.at[pl.ds((lo - low) * n + i * span, span)],
                send_sem=back_sem.at[2 * c], recv_sem=back_sem.at[2 * c + 1],
                device_id=device(d), device_id_type=MESH,
            ).start()

        each_partner(give)
        for k in range(span):
            back_ref[(lo - low) * n + k] = routed(me, k)
        if pick is None:
            peaks = jnp.transpose(peak)
        else:
            peaks = jnp.sum(jnp.where(pick[:count], peak, 0.0), axis=0, keepdims=True)
        scales = tabled(peaks * (1.0 / LEVELS), (lo, hi), scales)

    scale_v[...] = scales
    scale_ref[pl.ds(0, 1), :] = scale_v[pl.ds(me, 1), :]

    def give_scale(i):
        d = ahead_by(i)
        pltpu.make_async_remote_copy(
            src_ref=scale_v.at[pl.ds(d, 1)], dst_ref=scale_ref.at[pl.ds(i, 1)],
            send_sem=scale_sem.at[0], recv_sem=scale_sem.at[1],
            device_id=device(d), device_id_type=MESH,
        ).start()

    each_partner(give_scale)
    keep_more.wait()
    scaled = scale_ref.at[pl.ds(1, n - 1)]
    pltpu.make_async_copy(scaled, scaled, scale_sem.at[0]).wait()
    pltpu.make_async_copy(rest, rest, id_sem.at[0]).wait()
    for c, (lo, hi) in enumerate(parts):
        span, (send_f, recv_f, bp_v, send_b) = hi - lo, per_part[c]
        sent = send_f.at[pl.ds(span, (n - 1) * span)]
        pltpu.make_async_copy(sent, sent, fetch_sem.at[2 * c]).wait()
        given = send_b.at[pl.ds(span, (n - 1) * span)]
        pltpu.make_async_copy(given, given, back_sem.at[2 * c]).wait()
        landed = back_ref.at[pl.ds((lo - low) * n + span, (n - 1) * span)]
        pltpu.make_async_copy(landed, landed, back_sem.at[2 * c + 1]).wait()
    pltpu.make_async_copy(scaled, scaled, scale_sem.at[1]).wait()


def update_kernel(sizes, widths, *refs):
    block_rows, = sizes
    tables = 3 * len(widths)
    ratio_ref, out_hbm = refs[tables:tables + 2]
    out_ref, in_sem, out_sem = refs[-3:]
    smem = refs[tables + 2:-3]
    loads = []
    for j in range(len(widths)):
        loads += [
            pltpu.make_async_copy(refs[3 * j], smem[2 * j], in_sem.at[2 * j]),
            pltpu.make_async_copy(refs[3 * j + 1], smem[2 * j + 1], in_sem.at[2 * j + 1]),
        ]
    for load in loads:
        load.start()
    lane_tiles = out_ref.shape[1] // LANES
    per_group = SUBLANES // block_rows
    groups = out_ref.shape[0] // SUBLANES

    def clear(g, c):
        out_ref[pl.ds(pl.multiple_of(g * SUBLANES, SUBLANES), SUBLANES), :] = jnp.zeros((SUBLANES, out_ref.shape[1]), jnp.float32)
        return c

    lax.fori_loop(0, groups, clear, 0, unroll=8)
    for load in loads:
        load.wait()
    part_of_row = split(lax.broadcasted_iota(jnp.int32, (SUBLANES, LANES), 0), block_rows)[0]
    for j, wide in enumerate(widths):
        entry_s, scale_s, back_ref = smem[2 * j], smem[2 * j + 1], refs[3 * j + 2]

        def one(e, c):
            row, block, source = entry_s[0, e], entry_s[1, e], entry_s[2, e]
            i, k = split(source, wide)
            g, part = split(block, per_group)
            level = (back_ref[row].astype(jnp.int32) + HALF).astype(jnp.float32) * scale_s[i, k]
            rows = pl.ds(pl.multiple_of(g * SUBLANES, SUBLANES), SUBLANES)
            for h in range(lane_tiles):
                cols = slice(h * LANES, (h + 1) * LANES)
                piece = jnp.concatenate([level[h * block_rows:(h + 1) * block_rows]] * per_group, axis=0)
                out_ref[rows, cols] += jnp.where(part_of_row == part, piece * ratio_ref[rows, cols], 0.0)
            return c

        lax.fori_loop(0, entry_s[3, 0], one, 0)
    store = pltpu.make_async_copy(out_ref, out_hbm, out_sem)
    store.start()
    store.wait()


def local(image, sensitivity, system_blocks, tile_slab, tile_block, background):
    slabs, reps = lax.axis_size("slab"), lax.axis_size("rep")
    n = slabs * reps
    tiles, events, width = system_blocks.shape
    planes, rows, cols = image.shape
    block_rows = width // cols
    per_owner = rows // block_rows
    image2 = image.reshape(planes * rows, cols)
    sens2 = sensitivity.reshape(planes * rows, cols)
    sub = width // LANES
    blocks = planes * per_owner

    hbm = pl.BlockSpec(memory_space=pltpu.HBM)
    vmem = pl.BlockSpec(memory_space=pltpu.VMEM)

    def exchange(parts, collective_id):
        wide = parts[-1][1] - parts[0][0]
        rows_of_lists = 3 * SUBLANES * len(parts)
        buffers = []
        for lo, hi in parts:
            room = n * (hi - lo)
            buffers += [
                pltpu.VMEM((room, sub, LANES), jnp.bfloat16),
                pltpu.VMEM((room, sub, LANES), jnp.bfloat16),
                pltpu.VMEM((tiles, sub, LANES), jnp.int16),
                pltpu.VMEM((room, sub, LANES), jnp.int16),
            ]
        return pl.pallas_call(
            functools.partial(exchange_kernel, (n, reps, tiles, block_rows, per_owner), parts),
            out_shape=(
                pltpu.VMEM((SUBLANES, -(-n * wide // LANES) * LANES), jnp.int32),
                pltpu.VMEM((n, LANES), jnp.float32),
                pltpu.VMEM((n * wide, sub, LANES), jnp.int16),
                pltpu.VMEM(image2.shape, jnp.float32),
                pltpu.HBM((LANES,), jnp.int32),
            ),
            in_specs=[hbm] * 6,
            out_specs=(vmem, vmem, vmem, vmem, hbm),
            scratch_shapes=[
                pltpu.SMEM((LANES,), jnp.int32),
                pltpu.VMEM((n, LANES), jnp.int32),
                pltpu.VMEM((1, tiles), jnp.int32),
                pltpu.VMEM((1, tiles), jnp.int32),
                pltpu.VMEM(background.shape, jnp.bfloat16),
                pltpu.VMEM((n, LANES), jnp.float32),
                pltpu.VMEM(image2.shape, jnp.float32),
                pltpu.VMEM(image2.shape, jnp.float32),
                pltpu.VMEM((blocks, sub, LANES), jnp.bfloat16),
                pltpu.VMEM(system_blocks.shape, jnp.bfloat16),
                pltpu.VMEM((n, LANES), jnp.int32),
                pltpu.VMEM((rows_of_lists, LANES), jnp.int32),
                pltpu.SMEM((n, LANES), jnp.int32),
                pltpu.SMEM((rows_of_lists, LANES), jnp.int32),
                pltpu.SMEM((n, LANES), jnp.int32),
                pltpu.VMEM((tiles, sub, LANES), jnp.float32),
                pltpu.SemaphoreType.DMA((7,)),
                pltpu.SemaphoreType.DMA((2,)),
                pltpu.SemaphoreType.DMA((2,)),
                pltpu.SemaphoreType.DMA((2 * len(parts),)),
                pltpu.SemaphoreType.DMA((2 * len(parts),)),
                *buffers,
            ],
            compiler_params=pltpu.CompilerParams(
                collective_id=collective_id, has_side_effects=True, vmem_limit_bytes=VMEM_LIMIT
            ),
        )(tile_slab.reshape(1, tiles), tile_block.reshape(1, tiles), image2, sens2, system_blocks, background)

    def update(*results):
        tables = [table for result in results for table in result[:3]]
        widths = tuple(result[2].shape[0] // n for result in results)
        staged = []
        for entries, scale, _ in (result[:3] for result in results):
            staged += [pltpu.SMEM(entries.shape, jnp.int32), pltpu.SMEM(scale.shape, jnp.float32)]
        return pl.pallas_call(
            functools.partial(update_kernel, (block_rows,), widths),
            out_shape=pltpu.HBM(image2.shape, jnp.float32),
            in_specs=[vmem] * (len(tables) + 1),
            out_specs=hbm,
            scratch_shapes=[
                *staged,
                pltpu.VMEM(image2.shape, jnp.float32),
                pltpu.SemaphoreType.DMA((len(staged),)),
                pltpu.SemaphoreType.DMA,
            ],
            compiler_params=pltpu.CompilerParams(vmem_limit_bytes=VMEM_LIMIT),
        )(*tables, results[0][3])

    main = exchange(MAIN, 0)
    updated = lax.cond(
        main[4][0] > 0,
        lambda: update(main, exchange(REST, 1)),
        lambda: update(main),
    )
    return updated.reshape(image.shape)


def solution(mesh):
    return jax.shard_map(
        local,
        mesh=mesh,
        in_specs=(
            P("slab", "rep", None),
            P("slab", "rep", None),
            P(("slab", "rep"), None, None),
            P(("slab", "rep"), None),
            P(("slab", "rep")),
            P(("slab", "rep"), None),
        ),
        out_specs=P("slab", "rep", None),
        check_vma=False,
    )
```

```python
import functools

import jax
import jax.numpy as jnp
from jax import lax
from jax.experimental import pallas as pl
from jax.experimental.pallas import tpu as pltpu
from jax.sharding import PartitionSpec as P

CAP = 6
MAIN = ((0, 1), (1, 4))
REST = ((4, CAP),)
LEVELS = 65535.0
HALF = 32768
LANES = 128
SUBLANES = 8
MESH = pl.DeviceIdType.MESH
VMEM_LIMIT = 32 * 1024 * 1024


def split(x, size):
    if size & (size - 1):
        return x // size, x % size
    return x >> (size.bit_length() - 1), x & (size - 1)


def listed(tiles, part):
    lo, hi = part
    return tiles if lo == 0 else tiles * (hi - lo) // hi


def padded(count):
    return -(-count // SUBLANES) * SUBLANES


def exchange_kernel(sizes, parts, *refs):
    n, reps, tiles, block_rows, per_owner = sizes
    low, high = parts[0][0], parts[-1][1]
    wide = high - low
    slab_hbm, block_hbm, image_hbm, sens_hbm, sys_hbm, bg_hbm, entry_ref, scale_ref, back_ref, ratio_ref, more_ref = refs[:11]
    (
        turned_v, asked_ref, slab_v, block_v, bg_v, scale_v, image_v, sens_v, blocks_v, sys_v, mine_v, list_v, mine_s, list_s, asked_s, sums_v,
        local_sem, id_sem, scale_sem, fetch_sem, back_sem,
    ) = refs[11:32]
    per_part = [refs[32 + 4 * c:36 + 4 * c] for c in range(len(parts))]
    me = lax.axis_index("slab") * reps + lax.axis_index("rep")
    lane_tiles = image_v.shape[1] // LANES

    def device(d):
        return split(d, reps)

    load_sys = pltpu.make_async_copy(sys_hbm, sys_v, local_sem.at[0])
    load_image = pltpu.make_async_copy(image_hbm, image_v, local_sem.at[1])
    load_slab = pltpu.make_async_copy(slab_hbm, slab_v, local_sem.at[4])
    load_block = pltpu.make_async_copy(block_hbm, block_v, local_sem.at[5])
    load_bg = pltpu.make_async_copy(bg_hbm, bg_v, local_sem.at[6])
    load_sens = pltpu.make_async_copy(sens_hbm, sens_v, local_sem.at[4])
    for load in (load_slab, load_block, load_image, load_bg, load_sys):
        load.start()

    slabs = n // reps

    def each_partner(body):
        def line(j, carry):
            for s in range(slabs):
                body((slabs - 1 - s) * reps + reps - 1 - j)
            return carry

        lax.fori_loop(0, reps - 1, line, 0)
        for s in range(slabs - 1):
            body((slabs - 1 - s) * reps)

    barrier = pltpu.get_barrier_semaphore()

    def greet(i):
        pl.semaphore_signal(barrier, inc=1, device_id=device(me ^ i), device_id_type=MESH)

    each_partner(greet)
    load_slab.wait()
    load_block.wait()
    load_sens.start()
    block = block_v[...]
    plane, within = split(block, per_owner * reps)
    owner, offset = split(within, per_owner)
    key = slab_v[...] * reps + owner
    tile_lane = lax.broadcasted_iota(jnp.int32, (1, tiles), 1)
    value = (plane * per_owner + offset) * tiles + 1
    hot = key == lax.broadcasted_iota(jnp.int32, (n, tiles), 0)
    square = (tiles, tiles)
    earlier = lax.broadcasted_iota(jnp.int32, square, 0) < lax.broadcasted_iota(jnp.int32, square, 1)
    earlier = jnp.where(earlier, 1.0, 0.0).astype(jnp.bfloat16)

    def before(mask):
        ones = jnp.where(mask, 1.0, 0.0).astype(jnp.bfloat16)
        return jnp.dot(ones, earlier, preferred_element_type=jnp.float32).astype(jnp.int32)

    rank = before(hot)
    lane = lax.broadcasted_iota(jnp.int32, (n, LANES), 1)

    def tabled(row, part, table):
        for k in range(*part):
            picked = jnp.sum(jnp.where(hot & (rank == k), row, jnp.zeros_like(row)), axis=1, keepdims=True)
            table = jnp.where(lane == k - low, picked, table)
        return table

    own_rank = jnp.sum(jnp.where(hot, rank, 0), axis=0, keepdims=True)
    over = jnp.max(jnp.where(own_rank >= high, 1, 0), axis=1, keepdims=True)
    table = jnp.where(lane == wide, over, 0)
    hots = []
    for c, (lo, hi) in enumerate(parts):
        slot = (key ^ me) * (hi - lo) + own_rank - lo
        slot = jnp.clip(slot, 0, n * (hi - lo) - 1)
        row = 3 * SUBLANES * c
        if lo == 0:
            list_v[row:row + 1, 0:tiles] = slot
            hots.append(None)
            table = tabled(value + tile_lane, (lo, hi), table)
            continue
        room = padded(listed(tiles, (lo, hi)))
        mask = (own_rank >= lo) & (own_rank < hi)
        place = before(jnp.broadcast_to(mask, (room, tiles)))
        pick = (place == lax.broadcasted_iota(jnp.int32, (room, tiles), 0)) & mask
        hots.append(pick)
        tile_of = jnp.sum(jnp.where(pick, tile_lane, 0), axis=1, keepdims=True)
        slot_of = jnp.sum(jnp.where(pick, slot, 0), axis=1, keepdims=True)
        spread = lax.broadcasted_iota(jnp.int32, (room, LANES), 1)
        table = tabled(value + jnp.clip(place[0:1], 0, room - 1), (lo, hi), table)
        list_v[row + SUBLANES:row + SUBLANES + room, :] = jnp.where(spread == 0, tile_of, slot_of)
    mine_v[...] = table
    to_list = pltpu.make_async_copy(list_v, list_s, local_sem.at[2])
    to_list.start()
    to_mine = pltpu.make_async_copy(mine_v, mine_s, local_sem.at[3])
    to_mine.start()
    asked_ref[pl.ds(0, 1), :] = mine_v[pl.ds(me, 1), :]

    pl.semaphore_wait(barrier, n - 1)

    def send_ids(i):
        d = me ^ i
        pltpu.make_async_remote_copy(
            src_ref=mine_v.at[pl.ds(d, 1)], dst_ref=asked_ref.at[pl.ds(i, 1)],
            send_sem=id_sem.at[0], recv_sem=id_sem.at[1],
            device_id=device(d), device_id_type=MESH,
        ).start()

    each_partner(send_ids)
    to_list.wait()
    to_mine.wait()
    load_image.wait()
    per_group = SUBLANES // block_rows

    def cut(g, c):
        rows = image_v[pl.ds(pl.multiple_of(g * SUBLANES, SUBLANES), SUBLANES), :].astype(jnp.bfloat16).astype(jnp.float32)
        for u in range(per_group):
            blocks_v[g * per_group + u] = jnp.concatenate(
                [
                    rows[u * block_rows:(u + 1) * block_rows, h * LANES:(h + 1) * LANES]
                    for h in range(lane_tiles)
                ],
                axis=0,
            ).astype(jnp.bfloat16)
        return c

    groups = image_v.shape[0] // SUBLANES
    lax.fori_loop(0, groups, cut, 0, unroll=4)
    load_sens.wait()

    def divide(g, c):
        rows = pl.ds(pl.multiple_of(g * SUBLANES, SUBLANES), SUBLANES)
        ratio_ref[rows, :] = image_v[rows, :] / sens_v[rows, :]
        return c

    lax.fori_loop(0, groups, divide, 0, unroll=4)
    load_bg.wait()
    background = bg_v[...]
    columns = []
    for pick in hots:
        if pick is None:
            columns.append(jnp.transpose(background.astype(jnp.float32)))
        else:
            ones = jnp.where(pick, 1.0, 0.0)
            chosen = jnp.dot(ones.astype(jnp.bfloat16), background, preferred_element_type=jnp.float32)
            columns.append(jnp.transpose(chosen + (1.0 - jnp.sum(ones, axis=1, keepdims=True))))
    load_sys.wait()
    rest = asked_ref.at[pl.ds(1, n - 1)]
    pltpu.make_async_copy(rest, rest, id_sem.at[1]).wait()
    turned_v[:, 0:n] = jnp.transpose(asked_ref[...])[0:SUBLANES]
    to_asked = pltpu.make_async_copy(turned_v, asked_s, local_sem.at[2])
    to_asked.start()
    to_asked.wait()

    def served(i, k):
        return blocks_v[split(jnp.maximum(asked_s[k, i] - 1, 0), tiles)[0]]

    def fetch(c):
        lo, hi = parts[c]
        span, (send_f, recv_f, _, _) = hi - lo, per_part[c]
        for k in range(span):
            recv_f[k] = served(0, lo - low + k)

        def serve(i):
            for k in range(span):
                send_f[i * span + k] = served(i, lo - low + k)
            at = pl.ds(i * span, span)
            pltpu.make_async_remote_copy(
                src_ref=send_f.at[at], dst_ref=recv_f.at[at],
                send_sem=fetch_sem.at[2 * c], recv_sem=fetch_sem.at[2 * c + 1],
                device_id=device(me ^ i), device_id_type=MESH,
            ).start()

        each_partner(serve)

    for c in range(len(parts)):
        fetch(c)
    asked = asked_ref[...]
    flagged = jnp.max(jnp.where(lane == wide, asked, 0), axis=0, keepdims=True)
    more_ref[...] = jnp.broadcast_to(jnp.max(flagged, axis=1, keepdims=True), (1, LANES))
    below = lax.broadcasted_iota(jnp.int32, (n, n), 0) > lax.broadcasted_iota(jnp.int32, (n, n), 1)
    used = jnp.where((asked > 0) & (lane < wide), 1.0, 0.0).astype(jnp.bfloat16)
    ahead = jnp.dot(jnp.where(below, 1.0, 0.0).astype(jnp.bfloat16), used, preferred_element_type=jnp.float32).astype(jnp.int32)
    source = lax.broadcasted_iota(jnp.int32, (n, 1), 0)
    room = entry_ref.shape[1]
    position = lax.broadcasted_iota(jnp.int32, (n, room), 1)
    filled = jnp.zeros((1, 1), jnp.int32)
    entries = [jnp.zeros((1, room), jnp.int32) for _ in range(3)]
    for lo, hi in parts:
        for k in range(lo - low, hi - low):
            value_k = asked[:, k:k + 1]
            mine_k = (position == ahead[:, k:k + 1] + filled) & (value_k > 0)
            row_k = (lo - low) * n + source * (hi - lo) + k - (lo - low)
            facts = (row_k, split(value_k - 1, tiles)[0], source * wide + k)
            for f, fact in enumerate(facts):
                entries[f] += jnp.sum(jnp.where(mine_k, fact, 0), axis=0, keepdims=True)
            filled += jnp.sum(jnp.where(value_k > 0, 1, 0), axis=0, keepdims=True)
    for f, fact in enumerate(entries + [jnp.broadcast_to(filled, (1, room))]):
        entry_ref[f:f + 1, :] = fact

    pieces = block_rows * lane_tiles
    places = [(p % block_rows) * lane_tiles + p // block_rows for p in range(pieces)]
    scales = jnp.zeros((n, LANES), jnp.float32)
    for c, (lo, hi) in enumerate(parts):
        span, (send_f, recv_f, bp_v, send_b) = hi - lo, per_part[c]
        others = recv_f.at[pl.ds(span, (n - 1) * span)]
        pltpu.make_async_copy(others, others, fetch_sem.at[2 * c + 1]).wait()
        row, pick, count = 3 * SUBLANES * c, hots[c], listed(tiles, (lo, hi))
        if pick is None:
            chosen, cells_of = list(range(tiles)), [list_s[row, t] for t in range(tiles)]
        else:
            chosen = [jnp.clip(list_s[row + SUBLANES + j, 0], 0, tiles - 1) for j in range(count)]
            cells_of = [jnp.clip(list_s[row + SUBLANES + j, 1], 0, n * span - 1) for j in range(count)]
        forward = jnp.zeros(columns[c].shape, jnp.float32)
        column = lax.broadcasted_iota(jnp.int32, (1, forward.shape[1]), 1)
        for j in range(count):
            t = chosen[j]
            cells = recv_f[cells_of[j]].astype(jnp.float32)
            total = None
            for p, q in enumerate(places):
                term = sys_v[t, :, q * LANES:(q + 1) * LANES].astype(jnp.float32) * cells[p:p + 1, :]
                total = term if total is None else total + term
            forward = jnp.where(column == j, jnp.sum(total, axis=1, keepdims=True), forward)
        inverse = jnp.transpose(1.0 / (forward + columns[c])).astype(jnp.bfloat16)
        tops = []
        for j in range(count):
            back = jnp.dot(inverse, sys_v[chosen[j]], preferred_element_type=jnp.float32)
            tile = jnp.concatenate([back[j:j + 1, q * LANES:(q + 1) * LANES] for q in places], axis=0)
            sums_v[j] = tile
            tops.append(jnp.max(tile, axis=0, keepdims=True))
        peak = jnp.maximum(jnp.max(jnp.concatenate(tops, axis=0), axis=1, keepdims=True), 1e-33)
        gain = LEVELS / peak
        for j in range(count):
            level = jnp.round(sums_v[j] * gain[j:j + 1, :]).astype(jnp.int32) - HALF
            bp_v[j] = jnp.clip(level, -HALF, HALF - 1).astype(jnp.int16)

        def routed(d, k):
            return bp_v[split(jnp.maximum(mine_s[d, lo - low + k] - 1, 0), tiles)[1]]

        def give(i):
            d = me ^ i
            for k in range(span):
                send_b[i * span + k] = routed(d, k)
            pltpu.make_async_remote_copy(
                src_ref=send_b.at[pl.ds(i * span, span)], dst_ref=back_ref.at[pl.ds((lo - low) * n + i * span, span)],
                send_sem=back_sem.at[2 * c], recv_sem=back_sem.at[2 * c + 1],
                device_id=device(d), device_id_type=MESH,
            ).start()

        each_partner(give)
        for k in range(span):
            back_ref[(lo - low) * n + k] = routed(me, k)
        if pick is None:
            peaks = jnp.transpose(peak)
        else:
            peaks = jnp.sum(jnp.where(pick[:count], peak, 0.0), axis=0, keepdims=True)
        scales = tabled(peaks * (1.0 / LEVELS), (lo, hi), scales)

    scale_v[...] = scales
    scale_ref[pl.ds(0, 1), :] = scale_v[pl.ds(me, 1), :]

    def give_scale(i):
        d = me ^ i
        pltpu.make_async_remote_copy(
            src_ref=scale_v.at[pl.ds(d, 1)], dst_ref=scale_ref.at[pl.ds(i, 1)],
            send_sem=scale_sem.at[0], recv_sem=scale_sem.at[1],
            device_id=device(d), device_id_type=MESH,
        ).start()

    each_partner(give_scale)
    scaled = scale_ref.at[pl.ds(1, n - 1)]
    pltpu.make_async_copy(scaled, scaled, scale_sem.at[0]).wait()
    pltpu.make_async_copy(rest, rest, id_sem.at[0]).wait()
    for c, (lo, hi) in enumerate(parts):
        span, (send_f, recv_f, bp_v, send_b) = hi - lo, per_part[c]
        sent = send_f.at[pl.ds(span, (n - 1) * span)]
        pltpu.make_async_copy(sent, sent, fetch_sem.at[2 * c]).wait()
        given = send_b.at[pl.ds(span, (n - 1) * span)]
        pltpu.make_async_copy(given, given, back_sem.at[2 * c]).wait()
        landed = back_ref.at[pl.ds((lo - low) * n + span, (n - 1) * span)]
        pltpu.make_async_copy(landed, landed, back_sem.at[2 * c + 1]).wait()
    pltpu.make_async_copy(scaled, scaled, scale_sem.at[1]).wait()


def update_kernel(sizes, widths, *refs):
    block_rows, = sizes
    tables = 3 * len(widths)
    ratio_ref, out_hbm = refs[tables:tables + 2]
    out_ref, in_sem, out_sem = refs[-3:]
    staged = refs[tables + 2:-3]
    loads = []
    for j in range(len(widths)):
        entry_s, scale_s, turned_v = staged[3 * j:3 * j + 3]
        loads.append(pltpu.make_async_copy(refs[3 * j], entry_s, in_sem.at[2 * j]))
        loads[-1].start()
        scale_ref = refs[3 * j + 1]
        turned_v[:, 0:scale_ref.shape[0]] = jnp.transpose(scale_ref[...])[0:SUBLANES]
        loads.append(pltpu.make_async_copy(turned_v, scale_s, in_sem.at[2 * j + 1]))
        loads[-1].start()
    lane_tiles = out_ref.shape[1] // LANES
    per_group = SUBLANES // block_rows
    groups = out_ref.shape[0] // SUBLANES

    def clear(g, c):
        out_ref[pl.ds(pl.multiple_of(g * SUBLANES, SUBLANES), SUBLANES), :] = jnp.zeros((SUBLANES, out_ref.shape[1]), jnp.float32)
        return c

    lax.fori_loop(0, groups, clear, 0, unroll=8)
    for load in loads:
        load.wait()
    part_of_row = split(lax.broadcasted_iota(jnp.int32, (SUBLANES, LANES), 0), block_rows)[0]
    for j, wide in enumerate(widths):
        entry_s, scale_s, back_ref = staged[3 * j], staged[3 * j + 1], refs[3 * j + 2]

        def one(e, c):
            row, block, source = entry_s[0, e], entry_s[1, e], entry_s[2, e]
            i, k = split(source, wide)
            g, part = split(block, per_group)
            level = (back_ref[row].astype(jnp.int32) + HALF).astype(jnp.float32) * scale_s[k, i]
            rows = pl.ds(pl.multiple_of(g * SUBLANES, SUBLANES), SUBLANES)
            for h in range(lane_tiles):
                cols = slice(h * LANES, (h + 1) * LANES)
                piece = jnp.concatenate([level[h * block_rows:(h + 1) * block_rows]] * per_group, axis=0)
                out_ref[rows, cols] += jnp.where(part_of_row == part, piece * ratio_ref[rows, cols], 0.0)
            return c

        lax.fori_loop(0, entry_s[3, 0], one, 0)
    store = pltpu.make_async_copy(out_ref, out_hbm, out_sem)
    store.start()
    store.wait()


def local(image, sensitivity, system_blocks, tile_slab, tile_block, background):
    slabs, reps = lax.axis_size("slab"), lax.axis_size("rep")
    n = slabs * reps
    tiles, events, width = system_blocks.shape
    planes, rows, cols = image.shape
    block_rows = width // cols
    per_owner = rows // block_rows
    image2 = image.reshape(planes * rows, cols)
    sens2 = sensitivity.reshape(planes * rows, cols)
    sub = width // LANES
    blocks = planes * per_owner

    hbm = pl.BlockSpec(memory_space=pltpu.HBM)
    vmem = pl.BlockSpec(memory_space=pltpu.VMEM)

    def exchange(parts, collective_id):
        wide = parts[-1][1] - parts[0][0]
        rows_of_lists = 3 * SUBLANES * len(parts)
        buffers = []
        for lo, hi in parts:
            room = n * (hi - lo)
            buffers += [
                pltpu.VMEM((room, sub, LANES), jnp.bfloat16),
                pltpu.VMEM((room, sub, LANES), jnp.bfloat16),
                pltpu.VMEM((tiles, sub, LANES), jnp.int16),
                pltpu.VMEM((room, sub, LANES), jnp.int16),
            ]
        return pl.pallas_call(
            functools.partial(exchange_kernel, (n, reps, tiles, block_rows, per_owner), parts),
            out_shape=(
                pltpu.VMEM((SUBLANES, -(-n * wide // LANES) * LANES), jnp.int32),
                pltpu.VMEM((n, LANES), jnp.float32),
                pltpu.VMEM((n * wide, sub, LANES), jnp.int16),
                pltpu.VMEM(image2.shape, jnp.float32),
                pltpu.VMEM((1, LANES), jnp.int32),
            ),
            in_specs=[hbm] * 6,
            out_specs=(vmem,) * 5,
            scratch_shapes=[
                pltpu.VMEM((SUBLANES, max(n, LANES)), jnp.int32),
                pltpu.VMEM((n, LANES), jnp.int32),
                pltpu.VMEM((1, tiles), jnp.int32),
                pltpu.VMEM((1, tiles), jnp.int32),
                pltpu.VMEM(background.shape, jnp.bfloat16),
                pltpu.VMEM((n, LANES), jnp.float32),
                pltpu.VMEM(image2.shape, jnp.float32),
                pltpu.VMEM(image2.shape, jnp.float32),
                pltpu.VMEM((blocks, sub, LANES), jnp.bfloat16),
                pltpu.VMEM(system_blocks.shape, jnp.bfloat16),
                pltpu.VMEM((n, LANES), jnp.int32),
                pltpu.VMEM((rows_of_lists, LANES), jnp.int32),
                pltpu.SMEM((n, LANES), jnp.int32),
                pltpu.SMEM((rows_of_lists, LANES), jnp.int32),
                pltpu.SMEM((SUBLANES, max(n, LANES)), jnp.int32),
                pltpu.VMEM((tiles, sub, LANES), jnp.float32),
                pltpu.SemaphoreType.DMA((7,)),
                pltpu.SemaphoreType.DMA((2,)),
                pltpu.SemaphoreType.DMA((2,)),
                pltpu.SemaphoreType.DMA((2 * len(parts),)),
                pltpu.SemaphoreType.DMA((2 * len(parts),)),
                *buffers,
            ],
            compiler_params=pltpu.CompilerParams(
                collective_id=collective_id, has_side_effects=True, vmem_limit_bytes=VMEM_LIMIT
            ),
        )(tile_slab.reshape(1, tiles), tile_block.reshape(1, tiles), image2, sens2, system_blocks, background)

    def update(*results):
        tables = [table for result in results for table in result[:3]]
        widths = tuple(result[2].shape[0] // n for result in results)
        staged = []
        for entries, _, _ in (result[:3] for result in results):
            turned = (SUBLANES, max(n, LANES))
            staged += [
                pltpu.SMEM(entries.shape, jnp.int32),
                pltpu.SMEM(turned, jnp.float32),
                pltpu.VMEM(turned, jnp.float32),
            ]
        return pl.pallas_call(
            functools.partial(update_kernel, (block_rows,), widths),
            out_shape=pltpu.HBM(image2.shape, jnp.float32),
            in_specs=[vmem] * (len(tables) + 1),
            out_specs=hbm,
            scratch_shapes=[
                *staged,
                pltpu.VMEM(image2.shape, jnp.float32),
                pltpu.SemaphoreType.DMA((2 * len(results),)),
                pltpu.SemaphoreType.DMA,
            ],
            compiler_params=pltpu.CompilerParams(vmem_limit_bytes=VMEM_LIMIT),
        )(*tables, results[0][3])

    main = exchange(MAIN, 0)
    updated = lax.cond(
        main[4][0, 0] > 0,
        lambda: update(main, exchange(REST, 1)),
        lambda: update(main),
    )
    return updated.reshape(image.shape)


def solution(mesh):
    return jax.shard_map(
        local,
        mesh=mesh,
        in_specs=(
            P("slab", "rep", None),
            P("slab", "rep", None),
            P(("slab", "rep"), None, None),
            P(("slab", "rep"), None),
            P(("slab", "rep")),
            P(("slab", "rep"), None),
        ),
        out_specs=P("slab", "rep", None),
        check_vma=False,
    )
```

```python
import functools

import jax
import jax.numpy as jnp
from jax import lax
from jax.experimental import pallas as pl
from jax.experimental.pallas import tpu as pltpu
from jax.sharding import PartitionSpec as P

CAP = 6
MAIN = ((0, 1), (1, 2), (2, 4))
REST = ((4, CAP),)
LEVELS = 65535.0
MARGIN = 1.01
HALF = 32768
LANES = 128
SUBLANES = 8
MESH = pl.DeviceIdType.MESH
VMEM_LIMIT = 32 * 1024 * 1024


def split(x, size):
    if size & (size - 1):
        return x // size, x % size
    return x >> (size.bit_length() - 1), x & (size - 1)


def listed(tiles, part):
    lo, hi = part
    return tiles if lo == 0 else tiles * (hi - lo) // hi


def padded(count):
    return -(-count // SUBLANES) * SUBLANES


def exchange_kernel(sizes, parts, *refs):
    n, reps, tiles, block_rows, per_owner = sizes
    low, high = parts[0][0], parts[-1][1]
    wide = high - low
    slab_hbm, block_hbm, image_hbm, sens_hbm, sys_hbm, bg_hbm, entry_ref, scale_ref, back_ref, ratio_ref, more_ref = refs[:11]
    (
        turned_v, asked_ref, slab_v, block_v, bg_v, scale_v, image_v, sens_v, blocks_v, sys_v, mine_v, list_v, mine_s, list_s, asked_s,
        local_sem, id_sem, scale_sem, fetch_sem, back_sem,
    ) = refs[11:31]
    per_part = [refs[31 + 4 * c:35 + 4 * c] for c in range(len(parts))]
    me = lax.axis_index("slab") * reps + lax.axis_index("rep")
    lane_tiles = image_v.shape[1] // LANES

    def device(d):
        return split(d, reps)

    load_sys = pltpu.make_async_copy(sys_hbm, sys_v, local_sem.at[0])
    load_image = pltpu.make_async_copy(image_hbm, image_v, local_sem.at[1])
    load_slab = pltpu.make_async_copy(slab_hbm, slab_v, local_sem.at[4])
    load_block = pltpu.make_async_copy(block_hbm, block_v, local_sem.at[5])
    load_bg = pltpu.make_async_copy(bg_hbm, bg_v, local_sem.at[6])
    load_sens = pltpu.make_async_copy(sens_hbm, sens_v, local_sem.at[4])
    for load in (load_slab, load_block, load_image, load_bg, load_sys):
        load.start()

    slabs = n // reps

    def each_partner(body):
        def line(j, carry):
            for s in range(slabs):
                body((slabs - 1 - s) * reps + reps - 1 - j)
            return carry

        lax.fori_loop(0, reps - 1, line, 0)
        for s in range(slabs - 1):
            body((slabs - 1 - s) * reps)

    barrier = pltpu.get_barrier_semaphore()

    def greet(i):
        pl.semaphore_signal(barrier, inc=1, device_id=device(me ^ i), device_id_type=MESH)

    each_partner(greet)
    load_slab.wait()
    load_block.wait()
    load_sens.start()
    block = block_v[...]
    plane, within = split(block, per_owner * reps)
    owner, offset = split(within, per_owner)
    key = slab_v[...] * reps + owner
    tile_lane = lax.broadcasted_iota(jnp.int32, (1, tiles), 1)
    value = (plane * per_owner + offset) * tiles + 1
    hot = key == lax.broadcasted_iota(jnp.int32, (n, tiles), 0)
    square = (tiles, tiles)
    earlier = lax.broadcasted_iota(jnp.int32, square, 0) < lax.broadcasted_iota(jnp.int32, square, 1)
    earlier = jnp.where(earlier, 1.0, 0.0).astype(jnp.bfloat16)

    def before(mask):
        ones = jnp.where(mask, 1.0, 0.0).astype(jnp.bfloat16)
        return jnp.dot(ones, earlier, preferred_element_type=jnp.float32).astype(jnp.int32)

    rank = before(hot)
    lane = lax.broadcasted_iota(jnp.int32, (n, LANES), 1)

    def tabled(row, part, table):
        for k in range(*part):
            picked = jnp.sum(jnp.where(hot & (rank == k), row, jnp.zeros_like(row)), axis=1, keepdims=True)
            table = jnp.where(lane == k - low, picked, table)
        return table

    own_rank = jnp.sum(jnp.where(hot, rank, 0), axis=0, keepdims=True)
    over = jnp.max(jnp.where(own_rank >= high, 1, 0), axis=1, keepdims=True)
    table = jnp.where(lane == wide, over, 0)
    hots = []
    for c, (lo, hi) in enumerate(parts):
        slot = (key ^ me) * (hi - lo) + own_rank - lo
        slot = jnp.clip(slot, 0, n * (hi - lo) - 1)
        row = 3 * SUBLANES * c
        if lo == 0:
            list_v[row:row + 1, 0:tiles] = slot
            hots.append(None)
            table = tabled(value + tile_lane, (lo, hi), table)
            continue
        room = padded(listed(tiles, (lo, hi)))
        mask = (own_rank >= lo) & (own_rank < hi)
        place = before(jnp.broadcast_to(mask, (room, tiles)))
        pick = (place == lax.broadcasted_iota(jnp.int32, (room, tiles), 0)) & mask
        hots.append(pick)
        tile_of = jnp.sum(jnp.where(pick, tile_lane, 0), axis=1, keepdims=True)
        slot_of = jnp.sum(jnp.where(pick, slot, 0), axis=1, keepdims=True)
        spread = lax.broadcasted_iota(jnp.int32, (room, LANES), 1)
        table = tabled(value + jnp.clip(place[0:1], 0, room - 1), (lo, hi), table)
        list_v[row + SUBLANES:row + SUBLANES + room, :] = jnp.where(spread == 0, tile_of, slot_of)
    mine_v[...] = table
    to_list = pltpu.make_async_copy(list_v, list_s, local_sem.at[2])
    to_list.start()
    to_mine = pltpu.make_async_copy(mine_v, mine_s, local_sem.at[3])
    to_mine.start()
    asked_ref[pl.ds(0, 1), :] = mine_v[pl.ds(me, 1), :]

    pl.semaphore_wait(barrier, n - 1)

    def send_ids(i):
        d = me ^ i
        pltpu.make_async_remote_copy(
            src_ref=mine_v.at[pl.ds(d, 1)], dst_ref=asked_ref.at[pl.ds(i, 1)],
            send_sem=id_sem.at[0], recv_sem=id_sem.at[1],
            device_id=device(d), device_id_type=MESH,
        ).start()

    each_partner(send_ids)
    to_list.wait()
    to_mine.wait()
    load_image.wait()
    per_group = SUBLANES // block_rows

    def cut(g, c):
        rows = image_v[pl.ds(pl.multiple_of(g * SUBLANES, SUBLANES), SUBLANES), :].astype(jnp.bfloat16).astype(jnp.float32)
        for u in range(per_group):
            blocks_v[g * per_group + u] = jnp.concatenate(
                [
                    rows[u * block_rows:(u + 1) * block_rows, h * LANES:(h + 1) * LANES]
                    for h in range(lane_tiles)
                ],
                axis=0,
            ).astype(jnp.bfloat16)
        return c

    groups = image_v.shape[0] // SUBLANES
    lax.fori_loop(0, groups, cut, 0, unroll=4)
    load_bg.wait()
    background = bg_v[...].astype(jnp.float32)
    load_sys.wait()
    most = (MARGIN / background).astype(jnp.bfloat16)
    tops = []
    for t in range(tiles):
        bound = jnp.dot(most, sys_v[t], preferred_element_type=jnp.float32)[t:t + 1]
        top = bound[:, 0:LANES]
        for q in range(1, bound.shape[1] // LANES):
            top = jnp.maximum(top, bound[:, q * LANES:(q + 1) * LANES])
        tops.append(top)
    peak = jnp.maximum(jnp.max(jnp.concatenate(tops, axis=0), axis=1, keepdims=True), 1e-33)
    peaks = jnp.transpose(peak)
    scale_v[...] = tabled(peaks * (1.0 / LEVELS), (low, high), jnp.zeros((n, LANES), jnp.float32))
    scale_ref[pl.ds(0, 1), :] = scale_v[pl.ds(me, 1), :]

    def give_scale(i):
        d = me ^ i
        pltpu.make_async_remote_copy(
            src_ref=scale_v.at[pl.ds(d, 1)], dst_ref=scale_ref.at[pl.ds(i, 1)],
            send_sem=scale_sem.at[0], recv_sem=scale_sem.at[1],
            device_id=device(d), device_id_type=MESH,
        ).start()

    each_partner(give_scale)
    load_sens.wait()

    def divide(g, c):
        rows = pl.ds(pl.multiple_of(g * SUBLANES, SUBLANES), SUBLANES)
        ratio_ref[rows, :] = image_v[rows, :] / sens_v[rows, :]
        return c

    lax.fori_loop(0, groups, divide, 0, unroll=4)
    columns, gains = [], []
    for pick in hots:
        if pick is None:
            columns.append(jnp.transpose(background))
            gains.append(LEVELS / peak)
        else:
            ones = jnp.where(pick, 1.0, 0.0)
            chosen = jnp.dot(ones.astype(jnp.bfloat16), bg_v[...], preferred_element_type=jnp.float32)
            columns.append(jnp.transpose(chosen + (1.0 - jnp.sum(ones, axis=1, keepdims=True))))
            gains.append(jnp.sum(jnp.where(pick, LEVELS / peaks, 0.0), axis=1, keepdims=True))
    rest = asked_ref.at[pl.ds(1, n - 1)]
    pltpu.make_async_copy(rest, rest, id_sem.at[1]).wait()
    turned_v[:, 0:n] = jnp.transpose(asked_ref[...])[0:SUBLANES]
    to_asked = pltpu.make_async_copy(turned_v, asked_s, local_sem.at[2])
    to_asked.start()
    to_asked.wait()

    def served(i, k):
        return blocks_v[split(jnp.maximum(asked_s[k, i] - 1, 0), tiles)[0]]

    def fetch(c):
        lo, hi = parts[c]
        span, (send_f, recv_f, _, _) = hi - lo, per_part[c]
        for k in range(span):
            recv_f[k] = served(0, lo - low + k)

        def serve(i):
            for k in range(span):
                send_f[i * span + k] = served(i, lo - low + k)
            at = pl.ds(i * span, span)
            pltpu.make_async_remote_copy(
                src_ref=send_f.at[at], dst_ref=recv_f.at[at],
                send_sem=fetch_sem.at[2 * c], recv_sem=fetch_sem.at[2 * c + 1],
                device_id=device(me ^ i), device_id_type=MESH,
            ).start()

        each_partner(serve)

    for c in range(len(parts)):
        fetch(c)
    asked = asked_ref[...]
    flagged = jnp.max(jnp.where(lane == wide, asked, 0), axis=0, keepdims=True)
    more_ref[...] = jnp.broadcast_to(jnp.max(flagged, axis=1, keepdims=True), (1, LANES))
    below = lax.broadcasted_iota(jnp.int32, (n, n), 0) > lax.broadcasted_iota(jnp.int32, (n, n), 1)
    used = jnp.where((asked > 0) & (lane < wide), 1.0, 0.0).astype(jnp.bfloat16)
    ahead = jnp.dot(jnp.where(below, 1.0, 0.0).astype(jnp.bfloat16), used, preferred_element_type=jnp.float32).astype(jnp.int32)
    source = lax.broadcasted_iota(jnp.int32, (n, 1), 0)
    room = entry_ref.shape[1]
    position = lax.broadcasted_iota(jnp.int32, (n, room), 1)
    filled = jnp.zeros((1, 1), jnp.int32)
    entries = [jnp.zeros((1, room), jnp.int32) for _ in range(3)]
    for lo, hi in parts:
        for k in range(lo - low, hi - low):
            value_k = asked[:, k:k + 1]
            mine_k = (position == ahead[:, k:k + 1] + filled) & (value_k > 0)
            row_k = (lo - low) * n + source * (hi - lo) + k - (lo - low)
            facts = (row_k, split(value_k - 1, tiles)[0], source * wide + k)
            for f, fact in enumerate(facts):
                entries[f] += jnp.sum(jnp.where(mine_k, fact, 0), axis=0, keepdims=True)
            filled += jnp.sum(jnp.where(value_k > 0, 1, 0), axis=0, keepdims=True)
    for f, fact in enumerate(entries + [jnp.broadcast_to(filled, (1, room))]):
        entry_ref[f:f + 1, :] = fact

    pieces = block_rows * lane_tiles
    places = [(p % block_rows) * lane_tiles + p // block_rows for p in range(pieces)]
    for c, (lo, hi) in enumerate(parts):
        span, (send_f, recv_f, bp_v, send_b) = hi - lo, per_part[c]
        others = recv_f.at[pl.ds(span, (n - 1) * span)]
        pltpu.make_async_copy(others, others, fetch_sem.at[2 * c + 1]).wait()
        row, pick, count = 3 * SUBLANES * c, hots[c], listed(tiles, (lo, hi))
        if pick is None:
            chosen, cells_of = list(range(tiles)), [list_s[row, t] for t in range(tiles)]
        else:
            chosen = [jnp.clip(list_s[row + SUBLANES + j, 0], 0, tiles - 1) for j in range(count)]
            cells_of = [jnp.clip(list_s[row + SUBLANES + j, 1], 0, n * span - 1) for j in range(count)]
        forward = jnp.zeros(columns[c].shape, jnp.float32)
        column = lax.broadcasted_iota(jnp.int32, (1, forward.shape[1]), 1)
        for j in range(count):
            t = chosen[j]
            cells = recv_f[cells_of[j]].astype(jnp.float32)
            total = None
            for p, q in enumerate(places):
                term = sys_v[t, :, q * LANES:(q + 1) * LANES].astype(jnp.float32) * cells[p:p + 1, :]
                total = term if total is None else total + term
            forward = jnp.where(column == j, jnp.sum(total, axis=1, keepdims=True), forward)
        inverse = jnp.transpose(1.0 / (forward + columns[c])).astype(jnp.bfloat16)
        for j in range(count):
            back = jnp.dot(inverse, sys_v[chosen[j]], preferred_element_type=jnp.float32)
            tile = jnp.concatenate([back[j:j + 1, q * LANES:(q + 1) * LANES] for q in places], axis=0)
            level = jnp.round(tile * gains[c][j:j + 1, :]).astype(jnp.int32) - HALF
            bp_v[j] = jnp.clip(level, -HALF, HALF - 1).astype(jnp.int16)

        def routed(d, k):
            return bp_v[split(jnp.maximum(mine_s[d, lo - low + k] - 1, 0), tiles)[1]]

        def give(i):
            d = me ^ i
            for k in range(span):
                send_b[i * span + k] = routed(d, k)
            pltpu.make_async_remote_copy(
                src_ref=send_b.at[pl.ds(i * span, span)], dst_ref=back_ref.at[pl.ds((lo - low) * n + i * span, span)],
                send_sem=back_sem.at[2 * c], recv_sem=back_sem.at[2 * c + 1],
                device_id=device(d), device_id_type=MESH,
            ).start()

        each_partner(give)
        for k in range(span):
            back_ref[(lo - low) * n + k] = routed(me, k)
    scaled = scale_ref.at[pl.ds(1, n - 1)]
    pltpu.make_async_copy(scaled, scaled, scale_sem.at[0]).wait()
    pltpu.make_async_copy(rest, rest, id_sem.at[0]).wait()
    for c, (lo, hi) in enumerate(parts):
        span, (send_f, recv_f, bp_v, send_b) = hi - lo, per_part[c]
        sent = send_f.at[pl.ds(span, (n - 1) * span)]
        pltpu.make_async_copy(sent, sent, fetch_sem.at[2 * c]).wait()
        given = send_b.at[pl.ds(span, (n - 1) * span)]
        pltpu.make_async_copy(given, given, back_sem.at[2 * c]).wait()
        landed = back_ref.at[pl.ds((lo - low) * n + span, (n - 1) * span)]
        pltpu.make_async_copy(landed, landed, back_sem.at[2 * c + 1]).wait()
    pltpu.make_async_copy(scaled, scaled, scale_sem.at[1]).wait()


def update_kernel(sizes, widths, *refs):
    block_rows, = sizes
    tables = 3 * len(widths)
    ratio_ref, out_hbm = refs[tables:tables + 2]
    out_ref, in_sem, out_sem = refs[-3:]
    staged = refs[tables + 2:-3]
    loads = []
    for j in range(len(widths)):
        entry_s, scale_s, turned_v = staged[3 * j:3 * j + 3]
        loads.append(pltpu.make_async_copy(refs[3 * j], entry_s, in_sem.at[2 * j]))
        loads[-1].start()
        scale_ref = refs[3 * j + 1]
        turned_v[:, 0:scale_ref.shape[0]] = jnp.transpose(scale_ref[...])[0:SUBLANES]
        loads.append(pltpu.make_async_copy(turned_v, scale_s, in_sem.at[2 * j + 1]))
        loads[-1].start()
    lane_tiles = out_ref.shape[1] // LANES
    per_group = SUBLANES // block_rows
    groups = out_ref.shape[0] // SUBLANES

    def clear(g, c):
        out_ref[pl.ds(pl.multiple_of(g * SUBLANES, SUBLANES), SUBLANES), :] = jnp.zeros((SUBLANES, out_ref.shape[1]), jnp.float32)
        return c

    lax.fori_loop(0, groups, clear, 0, unroll=8)
    for load in loads:
        load.wait()
    part_of_row = split(lax.broadcasted_iota(jnp.int32, (SUBLANES, LANES), 0), block_rows)[0]
    for j, wide in enumerate(widths):
        entry_s, scale_s, back_ref = staged[3 * j], staged[3 * j + 1], refs[3 * j + 2]

        def one(e, c):
            row, block, source = entry_s[0, e], entry_s[1, e], entry_s[2, e]
            i, k = split(source, wide)
            g, part = split(block, per_group)
            level = (back_ref[row].astype(jnp.int32) + HALF).astype(jnp.float32) * scale_s[k, i]
            rows = pl.ds(pl.multiple_of(g * SUBLANES, SUBLANES), SUBLANES)
            for h in range(lane_tiles):
                cols = slice(h * LANES, (h + 1) * LANES)
                piece = jnp.concatenate([level[h * block_rows:(h + 1) * block_rows]] * per_group, axis=0)
                out_ref[rows, cols] += jnp.where(part_of_row == part, piece * ratio_ref[rows, cols], 0.0)
            return c

        lax.fori_loop(0, entry_s[3, 0], one, 0)
    store = pltpu.make_async_copy(out_ref, out_hbm, out_sem)
    store.start()
    store.wait()


def local(image, sensitivity, system_blocks, tile_slab, tile_block, background):
    slabs, reps = lax.axis_size("slab"), lax.axis_size("rep")
    n = slabs * reps
    tiles, events, width = system_blocks.shape
    planes, rows, cols = image.shape
    block_rows = width // cols
    per_owner = rows // block_rows
    image2 = image.reshape(planes * rows, cols)
    sens2 = sensitivity.reshape(planes * rows, cols)
    sub = width // LANES
    blocks = planes * per_owner

    hbm = pl.BlockSpec(memory_space=pltpu.HBM)
    vmem = pl.BlockSpec(memory_space=pltpu.VMEM)

    def exchange(parts, collective_id):
        wide = parts[-1][1] - parts[0][0]
        rows_of_lists = 3 * SUBLANES * len(parts)
        buffers = []
        for lo, hi in parts:
            room = n * (hi - lo)
            buffers += [
                pltpu.VMEM((room, sub, LANES), jnp.bfloat16),
                pltpu.VMEM((room, sub, LANES), jnp.bfloat16),
                pltpu.VMEM((tiles, sub, LANES), jnp.int16),
                pltpu.VMEM((room, sub, LANES), jnp.int16),
            ]
        return pl.pallas_call(
            functools.partial(exchange_kernel, (n, reps, tiles, block_rows, per_owner), parts),
            out_shape=(
                pltpu.VMEM((SUBLANES, -(-n * wide // LANES) * LANES), jnp.int32),
                pltpu.VMEM((n, LANES), jnp.float32),
                pltpu.VMEM((n * wide, sub, LANES), jnp.int16),
                pltpu.VMEM(image2.shape, jnp.float32),
                pltpu.VMEM((1, LANES), jnp.int32),
            ),
            in_specs=[hbm] * 6,
            out_specs=(vmem,) * 5,
            scratch_shapes=[
                pltpu.VMEM((SUBLANES, max(n, LANES)), jnp.int32),
                pltpu.VMEM((n, LANES), jnp.int32),
                pltpu.VMEM((1, tiles), jnp.int32),
                pltpu.VMEM((1, tiles), jnp.int32),
                pltpu.VMEM(background.shape, jnp.bfloat16),
                pltpu.VMEM((n, LANES), jnp.float32),
                pltpu.VMEM(image2.shape, jnp.float32),
                pltpu.VMEM(image2.shape, jnp.float32),
                pltpu.VMEM((blocks, sub, LANES), jnp.bfloat16),
                pltpu.VMEM(system_blocks.shape, jnp.bfloat16),
                pltpu.VMEM((n, LANES), jnp.int32),
                pltpu.VMEM((rows_of_lists, LANES), jnp.int32),
                pltpu.SMEM((n, LANES), jnp.int32),
                pltpu.SMEM((rows_of_lists, LANES), jnp.int32),
                pltpu.SMEM((SUBLANES, max(n, LANES)), jnp.int32),
                pltpu.SemaphoreType.DMA((7,)),
                pltpu.SemaphoreType.DMA((2,)),
                pltpu.SemaphoreType.DMA((2,)),
                pltpu.SemaphoreType.DMA((2 * len(parts),)),
                pltpu.SemaphoreType.DMA((2 * len(parts),)),
                *buffers,
            ],
            compiler_params=pltpu.CompilerParams(
                collective_id=collective_id, has_side_effects=True, vmem_limit_bytes=VMEM_LIMIT
            ),
        )(tile_slab.reshape(1, tiles), tile_block.reshape(1, tiles), image2, sens2, system_blocks, background)

    def update(*results):
        tables = [table for result in results for table in result[:3]]
        widths = tuple(result[2].shape[0] // n for result in results)
        staged = []
        for entries, _, _ in (result[:3] for result in results):
            turned = (SUBLANES, max(n, LANES))
            staged += [
                pltpu.SMEM(entries.shape, jnp.int32),
                pltpu.SMEM(turned, jnp.float32),
                pltpu.VMEM(turned, jnp.float32),
            ]
        return pl.pallas_call(
            functools.partial(update_kernel, (block_rows,), widths),
            out_shape=pltpu.HBM(image2.shape, jnp.float32),
            in_specs=[vmem] * (len(tables) + 1),
            out_specs=hbm,
            scratch_shapes=[
                *staged,
                pltpu.VMEM(image2.shape, jnp.float32),
                pltpu.SemaphoreType.DMA((2 * len(results),)),
                pltpu.SemaphoreType.DMA,
            ],
            compiler_params=pltpu.CompilerParams(vmem_limit_bytes=VMEM_LIMIT),
        )(*tables, results[0][3])

    main = exchange(MAIN, 0)
    updated = lax.cond(
        main[4][0, 0] > 0,
        lambda: update(main, exchange(REST, 1)),
        lambda: update(main),
    )
    return updated.reshape(image.shape)


def solution(mesh):
    return jax.shard_map(
        local,
        mesh=mesh,
        in_specs=(
            P("slab", "rep", None),
            P("slab", "rep", None),
            P(("slab", "rep"), None, None),
            P(("slab", "rep"), None),
            P(("slab", "rep")),
            P(("slab", "rep"), None),
        ),
        out_specs=P("slab", "rep", None),
        check_vma=False,
    )
```

```python
import functools

import jax
import jax.numpy as jnp
from jax import lax
from jax.experimental import pallas as pl
from jax.experimental.pallas import tpu as pltpu
from jax.sharding import PartitionSpec as P

CAP = 6
MAIN = ((0, 1), (1, 2), (2, 4))
REST = ((4, CAP),)
LEVELS = 65535.0
MARGIN = 1.01
STORES = 4
HALF = 32768
LANES = 128
SUBLANES = 8
MESH = pl.DeviceIdType.MESH
VMEM_LIMIT = 32 * 1024 * 1024


def split(x, size):
    if size & (size - 1):
        return x // size, x % size
    return x >> (size.bit_length() - 1), x & (size - 1)


def listed(tiles, part):
    lo, hi = part
    return tiles if lo == 0 else tiles * (hi - lo) // hi


def padded(count):
    return -(-count // SUBLANES) * SUBLANES


def exchange_kernel(sizes, parts, *refs):
    n, reps, tiles, block_rows, per_owner = sizes
    low, high = parts[0][0], parts[-1][1]
    wide = high - low
    slab_hbm, block_hbm, image_hbm, sens_hbm, sys_hbm, bg_hbm, entry_s, factor_s, back_ref, ratio_ref, more_ref = refs[:11]
    (
        turned_v, entry_ref, factor_ref, scale_ref, asked_ref, slab_v, block_v, bg_v, scale_v, image_v, sens_v, blocks_v, sys_v, mine_v, list_v, mine_s, list_s, asked_s,
        local_sem, id_sem, scale_sem, fetch_sem, back_sem,
    ) = refs[11:34]
    per_part = [refs[34 + 4 * c:38 + 4 * c] for c in range(len(parts))]
    me = lax.axis_index("slab") * reps + lax.axis_index("rep")
    lane_tiles = image_v.shape[1] // LANES

    def device(d):
        return split(d, reps)

    load_sys = pltpu.make_async_copy(sys_hbm, sys_v, local_sem.at[0])
    load_image = pltpu.make_async_copy(image_hbm, image_v, local_sem.at[1])
    load_slab = pltpu.make_async_copy(slab_hbm, slab_v, local_sem.at[4])
    load_block = pltpu.make_async_copy(block_hbm, block_v, local_sem.at[5])
    load_bg = pltpu.make_async_copy(bg_hbm, bg_v, local_sem.at[6])
    load_sens = pltpu.make_async_copy(sens_hbm, sens_v, local_sem.at[4])
    for load in (load_slab, load_block, load_image, load_bg, load_sys):
        load.start()

    slabs = n // reps

    def each_partner(body):
        def line(j, carry):
            for s in range(slabs):
                body((slabs - 1 - s) * reps + reps - 1 - j)
            return carry

        lax.fori_loop(0, reps - 1, line, 0)
        for s in range(slabs - 1):
            body((slabs - 1 - s) * reps)

    barrier = pltpu.get_barrier_semaphore()

    def greet(i):
        pl.semaphore_signal(barrier, inc=1, device_id=device(me ^ i), device_id_type=MESH)

    each_partner(greet)
    load_slab.wait()
    load_block.wait()
    load_sens.start()
    block = block_v[...]
    plane, within = split(block, per_owner * reps)
    owner, offset = split(within, per_owner)
    key = slab_v[...] * reps + owner
    tile_lane = lax.broadcasted_iota(jnp.int32, (1, tiles), 1)
    value = (plane * per_owner + offset) * tiles + 1
    hot = key == lax.broadcasted_iota(jnp.int32, (n, tiles), 0)
    square = (tiles, tiles)
    earlier = lax.broadcasted_iota(jnp.int32, square, 0) < lax.broadcasted_iota(jnp.int32, square, 1)
    earlier = jnp.where(earlier, 1.0, 0.0).astype(jnp.bfloat16)

    def before(mask):
        ones = jnp.where(mask, 1.0, 0.0).astype(jnp.bfloat16)
        return jnp.dot(ones, earlier, preferred_element_type=jnp.float32).astype(jnp.int32)

    rank = before(hot)
    lane = lax.broadcasted_iota(jnp.int32, (n, LANES), 1)

    def tabled(row, part, table):
        for k in range(*part):
            picked = jnp.sum(jnp.where(hot & (rank == k), row, jnp.zeros_like(row)), axis=1, keepdims=True)
            table = jnp.where(lane == k - low, picked, table)
        return table

    own_rank = jnp.sum(jnp.where(hot, rank, 0), axis=0, keepdims=True)
    over = jnp.max(jnp.where(own_rank >= high, 1, 0), axis=1, keepdims=True)
    table = jnp.where(lane == wide, over, 0)
    hots = []
    for c, (lo, hi) in enumerate(parts):
        slot = (key ^ me) * (hi - lo) + own_rank - lo
        slot = jnp.clip(slot, 0, n * (hi - lo) - 1)
        row = 3 * SUBLANES * c
        if lo == 0:
            list_v[row:row + 1, 0:tiles] = slot
            hots.append(None)
            table = tabled(value + tile_lane, (lo, hi), table)
            continue
        room = padded(listed(tiles, (lo, hi)))
        mask = (own_rank >= lo) & (own_rank < hi)
        place = before(jnp.broadcast_to(mask, (room, tiles)))
        pick = (place == lax.broadcasted_iota(jnp.int32, (room, tiles), 0)) & mask
        hots.append(pick)
        tile_of = jnp.sum(jnp.where(pick, tile_lane, 0), axis=1, keepdims=True)
        slot_of = jnp.sum(jnp.where(pick, slot, 0), axis=1, keepdims=True)
        spread = lax.broadcasted_iota(jnp.int32, (room, LANES), 1)
        table = tabled(value + jnp.clip(place[0:1], 0, room - 1), (lo, hi), table)
        list_v[row + SUBLANES:row + SUBLANES + room, :] = jnp.where(spread == 0, tile_of, slot_of)
    mine_v[...] = table
    to_list = pltpu.make_async_copy(list_v, list_s, local_sem.at[2])
    to_list.start()
    to_mine = pltpu.make_async_copy(mine_v, mine_s, local_sem.at[3])
    to_mine.start()
    asked_ref[pl.ds(0, 1), :] = mine_v[pl.ds(me, 1), :]

    pl.semaphore_wait(barrier, n - 1)

    def send_ids(i):
        d = me ^ i
        pltpu.make_async_remote_copy(
            src_ref=mine_v.at[pl.ds(d, 1)], dst_ref=asked_ref.at[pl.ds(i, 1)],
            send_sem=id_sem.at[0], recv_sem=id_sem.at[1],
            device_id=device(d), device_id_type=MESH,
        ).start()

    each_partner(send_ids)
    to_list.wait()
    to_mine.wait()
    load_image.wait()
    per_group = SUBLANES // block_rows

    def cut(g, c):
        rows = image_v[pl.ds(pl.multiple_of(g * SUBLANES, SUBLANES), SUBLANES), :].astype(jnp.bfloat16).astype(jnp.float32)
        for u in range(per_group):
            blocks_v[g * per_group + u] = jnp.concatenate(
                [
                    rows[u * block_rows:(u + 1) * block_rows, h * LANES:(h + 1) * LANES]
                    for h in range(lane_tiles)
                ],
                axis=0,
            ).astype(jnp.bfloat16)
        return c

    groups = image_v.shape[0] // SUBLANES
    lax.fori_loop(0, groups, cut, 0, unroll=4)
    load_bg.wait()
    background = bg_v[...].astype(jnp.float32)
    load_sys.wait()
    most = (MARGIN / background).astype(jnp.bfloat16)
    tops = []
    for t in range(tiles):
        bound = jnp.dot(most, sys_v[t], preferred_element_type=jnp.float32)[t:t + 1]
        top = bound[:, 0:LANES]
        for q in range(1, bound.shape[1] // LANES):
            top = jnp.maximum(top, bound[:, q * LANES:(q + 1) * LANES])
        tops.append(top)
    peak = jnp.maximum(jnp.max(jnp.concatenate(tops, axis=0), axis=1, keepdims=True), 1e-33)
    peaks = jnp.transpose(peak)
    scale_v[...] = tabled(peaks * (1.0 / LEVELS), (low, high), jnp.zeros((n, LANES), jnp.float32))
    scale_ref[pl.ds(0, 1), :] = scale_v[pl.ds(me, 1), :]

    def give_scale(i):
        d = me ^ i
        pltpu.make_async_remote_copy(
            src_ref=scale_v.at[pl.ds(d, 1)], dst_ref=scale_ref.at[pl.ds(i, 1)],
            send_sem=scale_sem.at[0], recv_sem=scale_sem.at[1],
            device_id=device(d), device_id_type=MESH,
        ).start()

    each_partner(give_scale)
    load_sens.wait()

    def divide(g, c):
        rows = pl.ds(pl.multiple_of(g * SUBLANES, SUBLANES), SUBLANES)
        ratio_ref[rows, :] = image_v[rows, :] / sens_v[rows, :]
        return c

    lax.fori_loop(0, groups, divide, 0, unroll=4)
    columns, gains = [], []
    for pick in hots:
        if pick is None:
            columns.append(jnp.transpose(background))
            gains.append(LEVELS / peak)
        else:
            ones = jnp.where(pick, 1.0, 0.0)
            chosen = jnp.dot(ones.astype(jnp.bfloat16), bg_v[...], preferred_element_type=jnp.float32)
            columns.append(jnp.transpose(chosen + (1.0 - jnp.sum(ones, axis=1, keepdims=True))))
            gains.append(jnp.sum(jnp.where(pick, LEVELS / peaks, 0.0), axis=1, keepdims=True))
    rest = asked_ref.at[pl.ds(1, n - 1)]
    pltpu.make_async_copy(rest, rest, id_sem.at[1]).wait()
    turned_v[:, 0:n] = jnp.transpose(asked_ref[...])[0:SUBLANES]
    to_asked = pltpu.make_async_copy(turned_v, asked_s, local_sem.at[2])
    to_asked.start()
    to_asked.wait()

    def served(i, k):
        return blocks_v[split(jnp.maximum(asked_s[k, i] - 1, 0), tiles)[0]]

    def fetch(c):
        lo, hi = parts[c]
        span, (send_f, recv_f, _, _) = hi - lo, per_part[c]
        for k in range(span):
            recv_f[k] = served(0, lo - low + k)

        def serve(i):
            for k in range(span):
                send_f[i * span + k] = served(i, lo - low + k)
            at = pl.ds(i * span, span)
            pltpu.make_async_remote_copy(
                src_ref=send_f.at[at], dst_ref=recv_f.at[at],
                send_sem=fetch_sem.at[2 * c], recv_sem=fetch_sem.at[2 * c + 1],
                device_id=device(me ^ i), device_id_type=MESH,
            ).start()

        each_partner(serve)

    for c in range(len(parts)):
        fetch(c)
    asked = asked_ref[...]
    flagged = jnp.max(jnp.where(lane == wide, asked, 0), axis=0, keepdims=True)
    more_ref[...] = jnp.broadcast_to(jnp.max(flagged, axis=1, keepdims=True), (1, LANES))
    below = lax.broadcasted_iota(jnp.int32, (n, n), 0) > lax.broadcasted_iota(jnp.int32, (n, n), 1)
    used = jnp.where((asked > 0) & (lane < wide), 1.0, 0.0).astype(jnp.bfloat16)
    ahead = jnp.dot(jnp.where(below, 1.0, 0.0).astype(jnp.bfloat16), used, preferred_element_type=jnp.float32).astype(jnp.int32)
    source = lax.broadcasted_iota(jnp.int32, (n, 1), 0)
    room = entry_ref.shape[1]
    position = lax.broadcasted_iota(jnp.int32, (n, room), 1)
    filled = jnp.zeros((1, 1), jnp.int32)
    entries = [jnp.zeros((1, room), jnp.int32) for _ in range(2)]
    for lo, hi in parts:
        for k in range(lo - low, hi - low):
            value_k = asked[:, k:k + 1]
            mine_k = (position == ahead[:, k:k + 1] + filled) & (value_k > 0)
            row_k = (lo - low) * n + source * (hi - lo) + k - (lo - low)
            facts = (row_k, split(value_k - 1, tiles)[0])
            for f, fact in enumerate(facts):
                entries[f] += jnp.sum(jnp.where(mine_k, fact, 0), axis=0, keepdims=True)
            filled += jnp.sum(jnp.where(value_k > 0, 1, 0), axis=0, keepdims=True)
    scaled = scale_ref.at[pl.ds(1, n - 1)]
    pltpu.make_async_copy(scaled, scaled, scale_sem.at[1]).wait()
    factor = jnp.zeros((1, room), jnp.float32)
    filled_by = jnp.zeros((1, 1), jnp.int32)
    for k in range(wide):
        value_k = asked[:, k:k + 1]
        mine_k = (position == ahead[:, k:k + 1] + filled_by) & (value_k > 0)
        factor += jnp.sum(jnp.where(mine_k, scale_ref[:, k:k + 1], 0.0), axis=0, keepdims=True)
        filled_by += jnp.sum(jnp.where(value_k > 0, 1, 0), axis=0, keepdims=True)
    factor_ref[0:1, :] = factor
    for f, fact in enumerate(entries + [jnp.broadcast_to(filled, (1, room))]):
        entry_ref[f:f + 1, :] = fact
    keep = [
        pltpu.make_async_copy(entry_ref, entry_s, local_sem.at[2]),
        pltpu.make_async_copy(factor_ref, factor_s, local_sem.at[3]),
    ]
    for copy in keep:
        copy.start()

    pieces = block_rows * lane_tiles
    places = [(p % block_rows) * lane_tiles + p // block_rows for p in range(pieces)]
    for c, (lo, hi) in enumerate(parts):
        span, (send_f, recv_f, bp_v, send_b) = hi - lo, per_part[c]
        others = recv_f.at[pl.ds(span, (n - 1) * span)]
        pltpu.make_async_copy(others, others, fetch_sem.at[2 * c + 1]).wait()
        row, pick, count = 3 * SUBLANES * c, hots[c], listed(tiles, (lo, hi))
        if pick is None:
            chosen, cells_of = list(range(tiles)), [list_s[row, t] for t in range(tiles)]
        else:
            chosen = [jnp.clip(list_s[row + SUBLANES + j, 0], 0, tiles - 1) for j in range(count)]
            cells_of = [jnp.clip(list_s[row + SUBLANES + j, 1], 0, n * span - 1) for j in range(count)]
        forward = jnp.zeros(columns[c].shape, jnp.float32)
        column = lax.broadcasted_iota(jnp.int32, (1, forward.shape[1]), 1)
        for j in range(count):
            t = chosen[j]
            cells = recv_f[cells_of[j]].astype(jnp.float32)
            total = None
            for p, q in enumerate(places):
                term = sys_v[t, :, q * LANES:(q + 1) * LANES].astype(jnp.float32) * cells[p:p + 1, :]
                total = term if total is None else total + term
            forward = jnp.where(column == j, jnp.sum(total, axis=1, keepdims=True), forward)
        inverse = jnp.transpose(1.0 / (forward + columns[c])).astype(jnp.bfloat16)
        for j in range(count):
            back = jnp.dot(inverse, sys_v[chosen[j]], preferred_element_type=jnp.float32)
            tile = jnp.concatenate([back[j:j + 1, q * LANES:(q + 1) * LANES] for q in places], axis=0)
            level = jnp.round(tile * gains[c][j:j + 1, :]).astype(jnp.int32) - HALF
            bp_v[j] = jnp.clip(level, -HALF, HALF - 1).astype(jnp.int16)

        def routed(d, k):
            return bp_v[split(jnp.maximum(mine_s[d, lo - low + k] - 1, 0), tiles)[1]]

        def give(i):
            d = me ^ i
            for k in range(span):
                send_b[i * span + k] = routed(d, k)
            pltpu.make_async_remote_copy(
                src_ref=send_b.at[pl.ds(i * span, span)], dst_ref=back_ref.at[pl.ds((lo - low) * n + i * span, span)],
                send_sem=back_sem.at[2 * c], recv_sem=back_sem.at[2 * c + 1],
                device_id=device(d), device_id_type=MESH,
            ).start()

        each_partner(give)
        for k in range(span):
            back_ref[(lo - low) * n + k] = routed(me, k)
    for copy in keep:
        copy.wait()
    pltpu.make_async_copy(scaled, scaled, scale_sem.at[0]).wait()
    pltpu.make_async_copy(rest, rest, id_sem.at[0]).wait()
    for c, (lo, hi) in enumerate(parts):
        span, (send_f, recv_f, bp_v, send_b) = hi - lo, per_part[c]
        sent = send_f.at[pl.ds(span, (n - 1) * span)]
        pltpu.make_async_copy(sent, sent, fetch_sem.at[2 * c]).wait()
        given = send_b.at[pl.ds(span, (n - 1) * span)]
        pltpu.make_async_copy(given, given, back_sem.at[2 * c]).wait()
        landed = back_ref.at[pl.ds((lo - low) * n + span, (n - 1) * span)]
        pltpu.make_async_copy(landed, landed, back_sem.at[2 * c + 1]).wait()


def update_kernel(block_rows, copies, *refs):
    tables = 3 * copies
    ratio_ref, out_hbm = refs[tables:tables + 2]
    out_ref, out_sem = refs[-2:]
    lane_tiles = out_ref.shape[1] // LANES
    per_group = SUBLANES // block_rows
    groups = out_ref.shape[0] // SUBLANES

    def clear(g, c):
        out_ref[pl.ds(pl.multiple_of(g * SUBLANES, SUBLANES), SUBLANES), :] = jnp.zeros((SUBLANES, out_ref.shape[1]), jnp.float32)
        return c

    lax.fori_loop(0, groups, clear, 0, unroll=8)
    part_of_row = split(lax.broadcasted_iota(jnp.int32, (SUBLANES, LANES), 0), block_rows)[0]
    for j in range(copies):
        entry_s, factor_s, back_ref = refs[3 * j:3 * j + 3]

        def one(e, c):
            row, block = entry_s[0, e], entry_s[1, e]
            g, part = split(block, per_group)
            level = (back_ref[row].astype(jnp.int32) + HALF).astype(jnp.float32) * factor_s[0, e]
            rows = pl.ds(pl.multiple_of(g * SUBLANES, SUBLANES), SUBLANES)
            for h in range(lane_tiles):
                cols = slice(h * LANES, (h + 1) * LANES)
                piece = jnp.concatenate([level[h * block_rows:(h + 1) * block_rows]] * per_group, axis=0)
                out_ref[rows, cols] += jnp.where(part_of_row == part, piece * ratio_ref[rows, cols], 0.0)
            return c

        lax.fori_loop(0, entry_s[2, 0], one, 0)
    stores = []
    for c in range(STORES):
        first, last = groups * c // STORES * SUBLANES, groups * (c + 1) // STORES * SUBLANES
        span = pl.ds(first, last - first)
        stores.append(pltpu.make_async_copy(out_ref.at[span], out_hbm.at[span], out_sem.at[c]))
        stores[-1].start()
    for store in stores:
        store.wait()


def local(image, sensitivity, system_blocks, tile_slab, tile_block, background):
    slabs, reps = lax.axis_size("slab"), lax.axis_size("rep")
    n = slabs * reps
    tiles, events, width = system_blocks.shape
    planes, rows, cols = image.shape
    block_rows = width // cols
    per_owner = rows // block_rows
    image2 = image.reshape(planes * rows, cols)
    sens2 = sensitivity.reshape(planes * rows, cols)
    sub = width // LANES
    blocks = planes * per_owner

    hbm = pl.BlockSpec(memory_space=pltpu.HBM)
    vmem = pl.BlockSpec(memory_space=pltpu.VMEM)
    smem = pl.BlockSpec(memory_space=pltpu.SMEM)

    def exchange(parts, collective_id):
        wide = parts[-1][1] - parts[0][0]
        room_of_entries = -(-n * wide // LANES) * LANES
        rows_of_lists = 3 * SUBLANES * len(parts)
        buffers = []
        for lo, hi in parts:
            room = n * (hi - lo)
            buffers += [
                pltpu.VMEM((room, sub, LANES), jnp.bfloat16),
                pltpu.VMEM((room, sub, LANES), jnp.bfloat16),
                pltpu.VMEM((tiles, sub, LANES), jnp.int16),
                pltpu.VMEM((room, sub, LANES), jnp.int16),
            ]
        return pl.pallas_call(
            functools.partial(exchange_kernel, (n, reps, tiles, block_rows, per_owner), parts),
            out_shape=(
                pltpu.SMEM((SUBLANES, room_of_entries), jnp.int32),
                pltpu.SMEM((SUBLANES, room_of_entries), jnp.float32),
                pltpu.VMEM((n * wide, sub, LANES), jnp.int16),
                pltpu.VMEM(image2.shape, jnp.float32),
                pltpu.VMEM((1, LANES), jnp.int32),
            ),
            in_specs=[hbm] * 6,
            out_specs=(smem,) * 2 + (vmem,) * 3,
            scratch_shapes=[
                pltpu.VMEM((SUBLANES, max(n, LANES)), jnp.int32),
                pltpu.VMEM((SUBLANES, room_of_entries), jnp.int32),
                pltpu.VMEM((SUBLANES, room_of_entries), jnp.float32),
                pltpu.VMEM((n, LANES), jnp.float32),
                pltpu.VMEM((n, LANES), jnp.int32),
                pltpu.VMEM((1, tiles), jnp.int32),
                pltpu.VMEM((1, tiles), jnp.int32),
                pltpu.VMEM(background.shape, jnp.bfloat16),
                pltpu.VMEM((n, LANES), jnp.float32),
                pltpu.VMEM(image2.shape, jnp.float32),
                pltpu.VMEM(image2.shape, jnp.float32),
                pltpu.VMEM((blocks, sub, LANES), jnp.bfloat16),
                pltpu.VMEM(system_blocks.shape, jnp.bfloat16),
                pltpu.VMEM((n, LANES), jnp.int32),
                pltpu.VMEM((rows_of_lists, LANES), jnp.int32),
                pltpu.SMEM((n, LANES), jnp.int32),
                pltpu.SMEM((rows_of_lists, LANES), jnp.int32),
                pltpu.SMEM((SUBLANES, max(n, LANES)), jnp.int32),
                pltpu.SemaphoreType.DMA((7,)),
                pltpu.SemaphoreType.DMA((2,)),
                pltpu.SemaphoreType.DMA((2,)),
                pltpu.SemaphoreType.DMA((2 * len(parts),)),
                pltpu.SemaphoreType.DMA((2 * len(parts),)),
                *buffers,
            ],
            compiler_params=pltpu.CompilerParams(
                collective_id=collective_id, has_side_effects=True, vmem_limit_bytes=VMEM_LIMIT
            ),
        )(tile_slab.reshape(1, tiles), tile_block.reshape(1, tiles), image2, sens2, system_blocks, background)

    def update(*results):
        tables = [table for result in results for table in result[:3]]
        return pl.pallas_call(
            functools.partial(update_kernel, block_rows, len(results)),
            out_shape=pltpu.HBM(image2.shape, jnp.float32),
            in_specs=[smem, smem, vmem] * len(results) + [vmem],
            out_specs=hbm,
            scratch_shapes=[
                pltpu.VMEM(image2.shape, jnp.float32),
                pltpu.SemaphoreType.DMA((STORES,)),
            ],
            compiler_params=pltpu.CompilerParams(vmem_limit_bytes=VMEM_LIMIT),
        )(*tables, results[0][3])

    main = exchange(MAIN, 0)
    updated = lax.cond(
        main[4][0, 0] > 0,
        lambda: update(main, exchange(REST, 1)),
        lambda: update(main),
    )
    return updated.reshape(image.shape)


def solution(mesh):
    return jax.shard_map(
        local,
        mesh=mesh,
        in_specs=(
            P("slab", "rep", None),
            P("slab", "rep", None),
            P(("slab", "rep"), None, None),
            P(("slab", "rep"), None),
            P(("slab", "rep")),
            P(("slab", "rep"), None),
        ),
        out_specs=P("slab", "rep", None),
        check_vma=False,
    )
```
